256 devices in a mesh: seq: 64 (over z, y, core), head: 4 (over x).
Axes of the slice: x: 4, y: 4, z: 8, core: 2. Of those that a mesh axis runs over, the one named last changes fastest.
Arguments:
- layer_in: bfloat16 [32768, 2048], P('seq', 'head'), may hold values from -6 to 6
- query_weight: bfloat16 [2048, 1024], P(None, 'head'), may hold values from -0.125 to 0.125
- key_weight: bfloat16 [2048, 1024], P(None, 'head'), may hold values from -0.125 to 0.125
- value_weight: bfloat16 [2048, 1024], P(None, 'head'), may hold values from -0.125 to 0.125
- gate_weight: bfloat16 [2048, 1024], P(None, 'head'), may hold values from -0.125 to 0.125
- beta_weight: bfloat16 [2048, 8], P(None, 'head'), may hold values from -0.125 to 0.125
- decay_weight: bfloat16 [2048, 8], P(None, 'head'), may hold values from -0.125 to 0.125
- conv_weight: float32 [4, 3, 1024], P(None, None, 'head'), may hold values from -3 to 3
- decay_log: float32 [8], P('head'), as said below
- beta_bias: float32 [8], P('head'), as said below
- decay_bias: float32 [8], P('head'), may hold values from -1 to 1
- norm_gain: float32 [128], replicated, may hold values from 0.1 to 1.9
- out_weight: bfloat16 [1024, 2048], P('head'), may hold values from -0.1875 to 0.1875
Outputs:
- layer_out: bfloat16 [32768, 2048], P('seq', 'head')
The draws below stay inside these ranges and needn't reach their ends.
Inputs may be any that keep to these rules, and one draw needn't show every extreme that they name: decay_log lies between log(0.1 / 32768) and log(0.05). beta_bias lies between log(0.5 * 128 / 32768) and 1.
All inputs are finite; a program needn't handle non-finite values.
Results may differ from the reference program's by a relative error of at most 0.0049.
Values may be sent and summed in bfloat16 or wider, within the bound.
A program may use at most 128 MiB of HBM per device.

```python
import jax
import jax.numpy as jnp
from jax import lax

D = 2048
HEADS = 8
HDIM = 128
CONV = 4
BLOCK = 128
TOKENS = 32768


def head_kinds(key):
    pair_count = HEADS // 2
    pick_one = jax.random.randint(jax.random.fold_in(key, 31), (pair_count,), 0, 2)
    rolled = jax.random.randint(jax.random.fold_in(key, 32), (pair_count,), 0, 100)
    limit = 25
    both_slow = rolled < limit
    first_slow = (pick_one == 0) | both_slow
    second_slow = (pick_one == 1) | both_slow
    return jnp.stack([first_slow, second_slow], axis=1).reshape(HEADS)


def draw_decay_log(key, part):
    slow_heads = head_kinds(key)
    spread = jax.random.uniform(jax.random.fold_in(key, 41), (HEADS,), jnp.float32)
    slow_rate = jnp.log((0.1 + 0.4 * spread) / TOKENS)
    fast_rate = jnp.log(0.02 + 0.03 * spread)
    return jnp.where(slow_heads, slow_rate, fast_rate).astype(jnp.float32)


def draw_beta_bias(key, part):
    slow_heads = head_kinds(key)
    spread = jax.random.uniform(jax.random.fold_in(key, 42), (HEADS,), jnp.float32)
    slow_bias = jnp.log((0.5 + 0.5 * spread) * HDIM / TOKENS)
    fast_bias = 2.0 * spread - 1.0
    return jnp.where(slow_heads, slow_bias, fast_bias).astype(jnp.float32)


def shard_levels(rng, shape, shards, smallest, high):
    loudness = 1.0
    for position, shards_of in shards:
        steps = jax.random.uniform(jax.random.fold_in(jax.random.fold_in(rng, 6), position), (shards_of,), jnp.float32, smallest / len(shards), high / len(shards))
        loudness = loudness * jnp.repeat(jnp.exp(steps), shape[position] // shards_of).reshape((-1,) + (1,) * (len(shape) - 1 - position))
    return loudness


def bell_draw(rng, extent, width, reach, pieces=(), kind=jnp.bfloat16):
    values = width * jax.random.normal(rng, extent, jnp.float32)
    if pieces:
        values = values * shard_levels(rng, extent, pieces, -0.22, 0.18)
    return jnp.clip(values, -reach, reach).astype(kind)


def setup_inputs(seed: int = 0) -> dict:
    seeds = jax.random.split(jax.random.key(seed), 14)
    layer_in = bell_draw(seeds[0], (TOKENS, D), 1.0, 6.0, ((0, 64), (1, 4)))
    query_weight = bell_draw(seeds[1], (D, HEADS * HDIM), D ** -0.5, 0.125, ((1, 4),))
    key_weight = bell_draw(seeds[2], (D, HEADS * HDIM), D ** -0.5, 0.125, ((1, 4),))
    value_weight = bell_draw(seeds[3], (D, HEADS * HDIM), D ** -0.5, 0.125, ((1, 4),))
    gate_weight = bell_draw(seeds[4], (D, HEADS * HDIM), D ** -0.5, 0.125, ((1, 4),))
    beta_weight = bell_draw(seeds[5], (D, HEADS), D ** -0.5, 0.125, ((1, 4),))
    decay_weight = bell_draw(seeds[6], (D, HEADS), D ** -0.5, 0.125, ((1, 4),))
    conv_weight = bell_draw(seeds[7], (CONV, 3, HEADS * HDIM), 0.5, 3.0, ((2, 4),), jnp.float32)
    decay_log = draw_decay_log(jax.random.fold_in(seeds[13], 71), 0)
    beta_bias = draw_beta_bias(jax.random.fold_in(seeds[13], 71), 0)
    decay_bias = jnp.clip(jax.random.uniform(seeds[10], (HEADS,), jnp.float32, -1.0, 1.0) * shard_levels(seeds[10], (HEADS,), ((0, 4),), -0.4, 0.0), -1.0, 1.0)
    norm_gain = jnp.clip(1.0 + 0.18 * jax.random.normal(seeds[11], (HDIM,), jnp.float32), 0.1, 1.9)
    out_weight = bell_draw(seeds[12], (HEADS * HDIM, D), (HEADS * HDIM) ** -0.5, 0.1875, ((0, 4),))
    return {"layer_in": layer_in, "query_weight": query_weight, "key_weight": key_weight, "value_weight": value_weight, "gate_weight": gate_weight, "beta_weight": beta_weight, "decay_weight": decay_weight, "conv_weight": conv_weight, "decay_log": decay_log, "beta_bias": beta_bias, "decay_bias": decay_bias, "norm_gain": norm_gain, "out_weight": out_weight}


exact_mode = lax.Precision.HIGHEST
norm_floor = 0.0001

def causal_conv(values, kernel):
    taps = kernel.shape[0]
    summed = kernel[0] * values
    for offset in range(1, taps):
        shifted = jnp.concatenate([jnp.zeros((offset, values.shape[1]), jnp.float32), values[:-offset]], axis=0)
        summed = summed + kernel[offset] * shifted
    return jax.nn.silu(summed)

def unit_rows(values):
    return values * lax.rsqrt(lax.optimization_barrier(jnp.sum(values * values, axis=-1, keepdims=True)) + 1.0)

def block_terms(queries, key_rows, values, beta_gate, log_decay):
    length = log_decay.shape[-1]
    running = jnp.cumsum(log_decay, axis=-1)
    row_index = lax.broadcasted_iota(jnp.int32, (length, length), 0)
    col_index = lax.broadcasted_iota(jnp.int32, (length, length), 1)
    within = row_index >= col_index
    before = row_index > col_index
    spread = running[..., :, None] - running[..., None, :]
    decay_matrix = jnp.where(within, jnp.exp(jnp.minimum(spread, 0.0)), 0.0)
    key_gram = jnp.einsum('...rd,...sd->...rs', key_rows, key_rows, precision=exact_mode)
    lower_part = jnp.where(before, beta_gate[..., :, None] * decay_matrix * key_gram, 0.0)
    system = lower_part + jnp.eye(length, dtype=jnp.float32)
    growth = jnp.exp(running)
    right_side = jnp.concatenate([beta_gate[..., None] * values, (beta_gate * growth)[..., None] * key_rows], axis=-1)
    solved = lax.linalg.triangular_solve(system, right_side, left_side=True, lower=True, unit_diagonal=True)
    value_dim = values.shape[-1]
    fixed_rows = solved[..., :value_dim]
    erased = solved[..., value_dim:]
    query_key = jnp.einsum('...rd,...sd->...rs', queries, key_rows, precision=exact_mode)
    mixing = jnp.where(within, decay_matrix * query_key, 0.0)
    local_out = jnp.einsum('...rs,...se->...re', mixing, fixed_rows, precision=exact_mode)
    reader = growth[..., None] * queries - jnp.einsum('...rs,...sd->...rd', mixing, erased, precision=exact_mode)
    tail_decay = jnp.exp(running[..., -1:] - running)
    weighted = tail_decay[..., None] * key_rows
    key_dim = key_rows.shape[-1]
    transit = jnp.exp(running[..., -1])[..., None, None] * jnp.eye(key_dim, dtype=jnp.float32) - jnp.einsum('...bd,...be->...de', weighted, erased, precision=exact_mode)
    carried = jnp.einsum('...bd,...be->...de', weighted, fixed_rows, precision=exact_mode)
    return (local_out, reader, transit, carried)

def reference(layer_in, query_weight, key_weight, value_weight, gate_weight, beta_weight, decay_weight, conv_weight, decay_log, beta_bias, decay_bias, norm_gain, out_weight):
    tokens = layer_in.shape[0]

    def project(weight):
        return jnp.dot(layer_in.astype(jnp.float32), weight.astype(jnp.float32), preferred_element_type=jnp.float32)
    mixed_query = causal_conv(project(query_weight), conv_weight[:, 0])
    mixed_key = causal_conv(project(key_weight), conv_weight[:, 1])
    mixed_value = causal_conv(project(value_weight), conv_weight[:, 2])
    queries = unit_rows(mixed_query.reshape(tokens, HEADS, HDIM))
    key_rows = unit_rows(mixed_key.reshape(tokens, HEADS, HDIM))
    values = mixed_value.reshape(tokens, HEADS, HDIM)
    beta_gate = jax.nn.sigmoid(project(beta_weight) + beta_bias)
    log_decay = -jnp.exp(decay_log) * jax.nn.softplus(project(decay_weight) + decay_bias)
    blocks = tokens // BLOCK

    def arrange(array):
        return array.reshape(blocks, BLOCK, HEADS, HDIM).transpose(0, 2, 1, 3)

    def arrange_gate(array):
        return array.reshape(blocks, BLOCK, HEADS).transpose(0, 2, 1)

    def advance(carry_state, inputs):
        local_out, reader, transit, carried = block_terms(*inputs)
        output = local_out + jnp.einsum('hrd,hde->hre', reader, carry_state, precision=exact_mode)
        carry_state = jnp.einsum('hde,hef->hdf', transit, carry_state, precision=exact_mode) + carried
        return (carry_state, output)
    zero_state = jnp.zeros((HEADS, HDIM, HDIM), jnp.float32)
    last_state, outputs = lax.scan(advance, zero_state, (arrange(queries), arrange(key_rows), arrange(values), arrange_gate(beta_gate), arrange_gate(log_decay)))
    head_out = outputs.transpose(0, 2, 1, 3).reshape(tokens, HEADS, HDIM)
    gate_rows = project(gate_weight).reshape(tokens, HEADS, HDIM)
    scaled = head_out * lax.rsqrt(lax.optimization_barrier(jnp.mean(head_out * head_out, axis=-1, keepdims=True)) + norm_floor)
    hidden = (scaled * norm_gain * jax.nn.silu(gate_rows)).reshape(tokens, HEADS * HDIM).astype(jnp.bfloat16)
    return jnp.dot(hidden.astype(jnp.float32), out_weight.astype(jnp.float32), preferred_element_type=jnp.float32).astype(jnp.bfloat16)
```

```python
import functools

import jax
import jax.numpy as jnp
from jax import lax
from jax.experimental import pallas as pl
from jax.experimental.pallas import tpu as pltpu
from jax.sharding import Mesh
from jax.sharding import PartitionSpec as P

F32 = jnp.float32
BF16 = jnp.bfloat16
MESH = pl.DeviceIdType.MESH
SEQ = ("z", "y", "c")
BLK = 128
HALF = BLK // 2
PRE = 16
NORM_FLOOR = 0.0001

NN = (((1,), (0,)), ((), ()))


def dot1(a, b):
    return lax.dot_general(a, b, NN, preferred_element_type=F32)


def halves(a):
    hi = a.astype(BF16)
    lo = (a - hi.astype(F32)).astype(BF16)
    return hi, lo


def left3(a):
    hi, lo = halves(a)
    return jnp.concatenate([hi, hi, lo], axis=1)


def right3(b):
    hi, lo = halves(b)
    return jnp.concatenate([hi, lo, hi], axis=0)


def dot3(a, b):
    return dot1(left3(a), right3(b))


def dot_exact_left(a_bf16, b):
    hi, lo = halves(b)
    return dot1(
        jnp.concatenate([a_bf16, a_bf16], axis=1), jnp.concatenate([hi, lo], axis=0)
    )


def sigmoid(v):
    return 1.0 / (1.0 + jnp.exp(-v))


def silu(v):
    return v / (1.0 + jnp.exp(-v))


def softplus(v):
    return jnp.maximum(v, 0.0) + jnp.log(1.0 + jnp.exp(-jnp.abs(v)))


def compose(later, earlier):
    l2, b2, c2 = later
    l1, b1, c1 = earlier
    moved = dot3(l2, jnp.concatenate([l1, b1], axis=1))
    width = l1.shape[1]
    return (
        c2[:, :width] * l1 + c1[:, :width] * l2 - moved[:, :width],
        c2[:, :width] * b1 + b2 - moved[:, width:],
        c1 * c2,
    )


def apply_map(m, state):
    l, b, c = m
    return c[:, : state.shape[1]] * state - dot3(l, state) + b


def pick(flag, m, other):
    return jax.tree.map(lambda a, b: jnp.where(flag, a, b), m, other)


def kernel(
    sizes,
    x_in,
    wq,
    wk,
    wv,
    wg,
    wbd,
    conv_w,
    decay_log,
    beta_bias,
    decay_bias,
    norm_gain,
    w_out,
    out,
    xg,
    w_all,
    col_w,
    state,
    logsum,
    prelim,
    gate,
    hg,
    sc_send,
    sc_recv,
    yb,
    zb,
    fin_send,
    sin,
    load_sem,
    pre_send,
    pre_recv,
    d_send,
    d_recv,
    f_send,
    f_recv,
    w_send,
    w_recv,
    c_send,
    c_recv,
    y_send,
    y_recv,
    z_send,
    z_recv,
    hd_send,
    hd_recv,
    hf_send,
    hf_recv,
):
    nz, ny, nx = sizes["z"], sizes["y"], sizes["x"]
    z = lax.axis_index("z")
    y = lax.axis_index("y")
    c = lax.axis_index("c")
    x = lax.axis_index("x")
    tokens = x_in.shape[0]
    feats = x_in.shape[1]
    chunks = tokens // BLK
    heads = 2
    width = heads * BLK
    right, left = lax.rem(x + 1, nx), lax.rem(x + nx - 1, nx)
    far = lax.rem(x + 2, nx)
    count = nz * ny * 2
    here = (z * ny + y) * 2 + c
    after = lax.rem(here + 1, count)
    prior = lax.rem(here + count - 1, count)

    def place(s, xx):
        return {"z": s // (ny * 2), "y": lax.rem(s // 2, ny), "c": lax.rem(s, 2), "x": xx}

    weights = (wq, wk, wv, wg)
    loads = [pltpu.make_async_copy(x_in, xg.at[x, pl.ds(PRE, tokens), :], load_sem.at[0])]
    loads[0].start()
    for i, w in enumerate(weights):
        cp = pltpu.make_async_copy(
            w, w_all.at[:, pl.ds(i * width, width)], load_sem.at[1 + i]
        )
        cp.start()
        loads.append(cp)
    cp = pltpu.make_async_copy(wbd, w_all.at[:, pl.ds(4 * width, BLK)], load_sem.at[5])
    cp.start()
    loads.append(cp)
    own_cols = pltpu.make_async_copy(
        w_out.at[:, pl.ds(pl.multiple_of(x * feats, feats), feats)],
        col_w.at[pl.ds(pl.multiple_of(x * width, width), width), :],
        load_sem.at[6],
    )
    own_cols.start()

    barrier = pltpu.get_barrier_semaphore()
    up_y, down_y = lax.rem(y + 1, ny), lax.rem(y + ny - 1, ny)
    up_z, down_z = lax.rem(z + 1, nz), lax.rem(z + nz - 1, nz)
    partners = [{"x": right}, {"x": left}, {"x": far}, {"c": 1 - c}]
    partners += [{"y": up_y}, {"y": down_y}, {"z": up_z}, {"z": down_z}]
    partners += [place(after, i) for i in range(nx)]
    partners += [place(prior, i) for i in range(nx)]
    for who in partners:
        pl.semaphore_signal(barrier, inc=1, device_id=who, device_id_type=MESH)

    state[...] = jnp.zeros_like(state)
    eye = (
        lax.broadcasted_iota(jnp.int32, (BLK, BLK), 0)
        == lax.broadcasted_iota(jnp.int32, (BLK, BLK), 1)
    ).astype(F32)
    for h in range(heads):
        state[h, :, 0:BLK] = eye
    logsum[...] = jnp.zeros_like(logsum)
    pl.semaphore_wait(barrier, len(partners))
    loads[0].wait()

    def remote(src, dst, send, recv, who):
        return pltpu.make_async_remote_copy(
            src_ref=src,
            dst_ref=dst,
            send_sem=send,
            recv_sem=recv,
            device_id=who,
            device_id_type=MESH,
        )


    def ring(buf, base, send, recv, relay_send, relay_recv):
        def direct(way, t):
            rows = pl.ds(pl.multiple_of(base + t * BLK, PRE), BLK)
            return remote(
                buf.at[x, rows, :],
                buf.at[x, rows, :],
                send.at[way, t],
                recv.at[way, t],
                {"x": (right, left)[way]},
            )

        def relay(way, t):
            rows = pl.ds(pl.multiple_of(base + t * BLK + way * HALF, PRE), HALF)
            source = (left, right)[way]
            return remote(
                buf.at[source, rows, :],
                buf.at[source, rows, :],
                relay_send.at[way, t],
                relay_recv.at[way, t],
                {"x": (right, left)[way]},
            )

        return direct, relay

    direct, relay = ring(xg, PRE, d_send, d_recv, f_send, f_recv)

    def pre_copy(i):
        return remote(
            xg.at[x, pl.ds(tokens, PRE), :],
            xg.at[x, pl.ds(0, PRE), :],
            pre_send.at[i],
            pre_recv.at[x],
            place(after, i),
        )

    for i in range(nx):
        pre_copy(i).start()
    for t in range(2):
        for way in range(2):
            direct(way, t).start()
    for cp in loads[1:]:
        cp.wait()

    row_i = lax.broadcasted_iota(jnp.int32, (BLK, BLK), 0)
    col_i = lax.broadcasted_iota(jnp.int32, (BLK, BLK), 1)
    differ = jnp.bitwise_xor(row_i, col_i)
    within = row_i >= col_i
    before = row_i > col_i

    lane = lax.broadcasted_iota(jnp.int32, (1, BLK), 1)
    bias_row = jnp.where(lane == 0, beta_bias[0], 0.0)
    bias_row = jnp.where(lane == 1, beta_bias[1], bias_row)
    bias_row = jnp.where(lane == 2, decay_bias[0], bias_row)
    bias_row = jnp.where(lane == 3, decay_bias[1], bias_row)
    rate_row = jnp.where(lane == 2, decay_log[0], -200.0)
    rate_row = jnp.exp(jnp.where(lane == 3, decay_log[1], rate_row))
    gain_row = norm_gain[...].reshape(1, BLK)

    def unit_rows(v):
        return v * lax.rsqrt(jnp.sum(v * v, axis=-1, keepdims=True) + 1.0)

    def chunk(t):
        start = pl.multiple_of(t * BLK, BLK)
        rows = pl.ds(start, BLK + PRE)
        xs = jnp.concatenate([xg[p, rows, :] for p in range(nx)], axis=1)
        first = jnp.logical_and(here == 0, t == 0)
        ext_row = lax.broadcasted_iota(jnp.int32, (BLK + PRE, 3 * width), 0)
        raw = dot1(xs, w_all[...])
        qkv = raw[:, 0 : 3 * width]
        qkv = jnp.where(jnp.logical_and(first, ext_row < PRE), 0.0, qkv)
        taps = [
            jnp.concatenate([conv_w[s, i : i + 1, :] for i in range(3)], axis=1)
            for s in range(4)
        ]
        mixed = taps[0] * qkv
        for s in range(1, 4):
            mixed = mixed + taps[s] * pltpu.roll(qkv, s, 0)
        mixed = silu(mixed[PRE:])
        out_rows = pl.ds(start, BLK)
        gates = silu(raw[PRE:, 3 * width : 4 * width])
        for h in range(heads):
            gate[out_rows, h * BLK : (h + 1) * BLK] = (
                gates[:, h * BLK : (h + 1) * BLK] * gain_row
            )
        small = raw[PRE:, 4 * width :] + bias_row
        betas = sigmoid(small)
        steps = -rate_row * softplus(small)
        s_hi = steps.astype(BF16)
        rest = steps - s_hi.astype(F32)
        s_mid = rest.astype(BF16)
        s_lo = (rest - s_mid.astype(F32)).astype(BF16)
        tri = within.astype(F32).astype(BF16)
        total = dot1(
            jnp.concatenate([tri, tri, tri], axis=1),
            jnp.concatenate([s_hi, s_mid, s_lo], axis=0),
        )
        total_t = jnp.transpose(total)
        both = []
        for h in range(heads):
            cols = slice(h * BLK, (h + 1) * BLK)
            q = unit_rows(mixed[:, h * BLK : (h + 1) * BLK])
            k = unit_rows(mixed[:, width + h * BLK : width + (h + 1) * BLK])
            v = mixed[:, 2 * width + h * BLK : 2 * width + (h + 1) * BLK]
            beta = betas[:, h : h + 1]
            run_c = total[:, 2 + h : 3 + h]
            run_r = total_t[2 + h : 3 + h, :]
            end = run_r[:, BLK - 1 : BLK]
            decay = jnp.where(within, jnp.exp(jnp.minimum(run_c - run_r, 0.0)), 0.0)
            kt = jnp.transpose(k)
            scores = dot3(jnp.concatenate([k, q], axis=0), kt)
            low = jnp.where(before, beta * decay * scores[:BLK], 0.0)
            mix = decay * scores[BLK:]
            grow = jnp.exp(run_c)
            ext = state[h]
            read = dot3(
                jnp.concatenate([(beta * grow) * k, grow * q], axis=0), ext
            )
            right_side = (
                jnp.concatenate([jnp.zeros_like(v), beta * v], axis=1) - read[:BLK]
            )
            both.append((low, mix, right_side, read[BLK:], kt, run_r, end, ext))
        inv = [
            jnp.where(row_i == col_i, 1.0, 0.0) - jnp.where(differ == 1, b[0], 0.0)
            for b in both
        ]
        w = 2
        while w < BLK:
            linking = jnp.logical_and(differ >= w, differ < 2 * w)
            inv3 = [right3(a) for a in inv]
            mids = [
                dot1(left3(jnp.where(linking, b[0], 0.0)), a)
                for b, a in zip(both, inv3)
            ]
            inv = [a - dot3(a, m) for a, m in zip(inv, mids)]
            w *= 2
        for h in range(heads):
            low, mix, right_side, carried, kt, run_r, end, ext = both[h]
            solved = dot3(inv[h], right_side)
            solved3 = right3(solved)
            prelim[h, out_rows, :] = carried + dot1(left3(mix), solved3)
            weighted = kt * jnp.exp(end - run_r)
            state[h] = jnp.exp(end) * ext + dot1(left3(weighted), solved3)
            logsum[h] = logsum[h] + jnp.broadcast_to(end, logsum.shape[1:])

    def step(t, carry):
        @pl.when(t < chunks)
        def _():
            direct(0, t).wait_recv()
            direct(1, t).wait_recv()
            relay(0, t).start()
            relay(1, t).start()

        @pl.when(t < chunks - 2)
        def _():
            direct(0, t + 2).start()
            direct(1, t + 2).start()

        @pl.when(t == 0)
        def _():
            for i in range(nx):
                remote(
                    xg.at[i, pl.ds(tokens, PRE), :],
                    xg.at[i, pl.ds(0, PRE), :],
                    pre_send.at[i],
                    pre_recv.at[i],
                    place(after, i),
                ).wait_recv()

        @pl.when(t > 0)
        def _():
            relay(0, t - 1).wait_recv()
            relay(1, t - 1).wait_recv()
            chunk(t - 1)

        return carry

    lax.fori_loop(0, chunks + 1, step, 0)

    def columns(j):
        who = lax.rem(x + j, nx)
        return remote(
            w_out.at[:, pl.ds(pl.multiple_of(who * feats, feats), feats)],
            col_w.at[pl.ds(pl.multiple_of(x * width, width), width), :],
            w_send.at[j - 1],
            w_recv.at[j - 1],
            {"x": who},
        )

    for j in range(1, nx):
        columns(j).start()

    def own_map(h):
        ext = state[h]
        keep = jnp.exp(logsum[h, 0:1, :])
        return (keep[:, :BLK] * eye - ext[:, :BLK], ext[:, BLK:], keep)

    sl, sb, skeep = own_map(1 - c)
    sc_send[0:BLK, 0:BLK] = sl
    sc_send[0:BLK, BLK:] = sb
    sc_send[BLK:, :] = jnp.broadcast_to(skeep, (8, 2 * BLK))
    swap = remote(sc_send, sc_recv, c_send.at[0], c_recv.at[0], {"c": 1 - c})
    swap.start()
    mine = own_map(c)
    swap.wait()
    other = (sc_recv[0:BLK, 0:BLK], sc_recv[0:BLK, BLK:], sc_recv[BLK : BLK + 1, :])
    is_first = c == 0
    map0 = pick(is_first, mine, other)
    map1 = pick(is_first, other, mine)
    chip_map = compose(map1, map0)

    def put(buf, slot, m):
        l, b, keep = m
        buf[slot, 0:BLK, 0:BLK] = l.astype(BF16)
        buf[slot, 0:BLK, BLK:] = b.astype(BF16)
        hi, lo = halves(keep)
        tail = lax.broadcasted_iota(jnp.int32, (PRE, 2 * BLK), 0)
        buf[slot, BLK:, :] = jnp.where(
            tail == 0, jnp.broadcast_to(hi.astype(F32), (PRE, 2 * BLK)),
            jnp.broadcast_to(lo.astype(F32), (PRE, 2 * BLK)),
        ).astype(BF16)

    def get(buf, slot):
        tail = buf[slot, BLK:, :].astype(F32)
        return (
            buf[slot, 0:BLK, 0:BLK].astype(F32),
            buf[slot, 0:BLK, BLK:].astype(F32),
            tail[0:1] + tail[1:2],
        )

    put(yb, y, chip_map)

    def y_copy(slot, j, who):
        return remote(yb.at[slot], yb.at[slot], y_send.at[j], y_recv.at[j], {"y": who})

    y1 = y_copy(y, 0, up_y)
    y2 = y_copy(y, 1, down_y)
    y1.start()
    y2.start()
    y1.wait_recv()
    y3 = y_copy(down_y, 2, up_y)
    y3.start()
    y2.wait_recv()
    y3.wait_recv()
    zero = jnp.zeros((BLK, BLK), F32)
    one_row = jnp.ones((1, 2 * BLK), F32)
    identity = (zero, zero, one_row)
    maps = [get(yb, j) for j in range(ny)]
    run = maps[0]
    before_row = pick(y == 0, identity, run)
    for j in range(1, ny):
        before_row = pick(y == j, run, before_row) if j > 1 else before_row
        run = compose(maps[j], run)

    put(zb, z, run)

    def z_copy(slot, j, who):
        return remote(zb.at[slot], zb.at[slot], z_send.at[j], z_recv.at[j], {"z": who})

    ups, downs = nz // 2, nz - 1 - nz // 2
    near = identity
    low_state = zero
    flights = []
    for j in range(ups):
        cp = z_copy(lax.rem(z + nz - j, nz), j, up_z)
        cp.start()
        flights.append(cp)
        dn = None
        if j < downs:
            dn = z_copy(lax.rem(z + j, nz), ups + j, down_z)
            dn.start()
            flights.append(dn)
        if j > 0:
            got = pick(z - j >= 0, get(zb, lax.rem(z + nz - j, nz)), identity)
            near = compose(near, got)
            if j <= downs:
                got = pick(z + j - nz >= 0, get(zb, lax.rem(z + j, nz)), identity)
                low_state = apply_map(got, low_state)
        cp.wait_recv()
        if dn is not None:
            dn.wait_recv()
    got = pick(z - ups >= 0, get(zb, lax.rem(z + nz - ups, nz)), identity)
    row_state = apply_map(near, apply_map(got, low_state))
    chip_state = apply_map(before_row, row_state)
    later_state = apply_map(map0, chip_state)
    sin[c] = jnp.where(is_first, chip_state, later_state)
    fin_send[...] = jnp.where(is_first, later_state, chip_state)
    give = remote(fin_send, sin.at[c], c_send.at[1], c_recv.at[1], {"c": 1 - c})
    give.start()
    give.wait()

    h_direct, h_relay = ring(hg, 0, hd_send, hd_recv, hf_send, hf_recv)
    starts = [right3(sin[h]) for h in range(heads)]
    for t in range(chunks):
        rows = slice(t * BLK, (t + 1) * BLK)
        for h in range(heads):
            part = prelim[h, rows, :]
            head_out = dot1(left3(part[:, :BLK]), starts[h]) + part[:, BLK:]
            scaled = head_out * lax.rsqrt(
                jnp.mean(head_out * head_out, axis=-1, keepdims=True) + NORM_FLOOR
            )
            cols = slice(h * BLK, (h + 1) * BLK)
            hg[x, rows, cols] = (scaled * gate[rows, cols]).astype(BF16)
        for way in range(2):
            h_direct(way, t).start()
    for t in range(chunks):
        for way in range(2):
            h_direct(way, t).wait_recv()
            h_relay(way, t).start()
    own_cols.wait()
    for j in range(1, nx):
        columns(j).wait_recv()
    for t in range(chunks):
        rows = slice(t * BLK, (t + 1) * BLK)
        for way in range(2):
            h_relay(way, t).wait_recv()
        rows_all = jnp.concatenate([hg[p, rows, :] for p in range(nx)], axis=1)
        out[rows, :] = dot1(rows_all, col_w[...]).astype(BF16)

    for i in range(nx):
        pre_copy(i).wait_send()
    for t in range(chunks):
        for way in range(2):
            direct(way, t).wait_send()
            relay(way, t).wait_send()
            h_direct(way, t).wait_send()
            h_relay(way, t).wait_send()
    for j in range(1, nx):
        columns(j).wait_send()
    for cp in (y1, y2, y3):
        cp.wait_send()
    for cp in flights:
        cp.wait_send()


def on_device(
    sizes,
    layer_in,
    query_weight,
    key_weight,
    value_weight,
    gate_weight,
    beta_weight,
    decay_weight,
    conv_weight,
    decay_log,
    beta_bias,
    decay_bias,
    norm_gain,
    out_weight,
):
    tokens, feats = layer_in.shape
    depth, width = query_weight.shape
    nz, ny, nx = sizes["z"], sizes["y"], sizes["x"]
    chunks = tokens // BLK
    heads = 2
    small = jnp.concatenate(
        [
            beta_weight,
            decay_weight,
            jnp.zeros((depth, BLK - 2 * heads), BF16),
        ],
        axis=1,
    )
    anyspace = pl.BlockSpec(memory_space=pl.ANY)
    vmem = pl.BlockSpec(memory_space=pltpu.VMEM)
    smem = pl.BlockSpec(memory_space=pltpu.SMEM)
    dma = pltpu.SemaphoreType.DMA
    zc = nz - 1
    return pl.pallas_call(
        functools.partial(kernel, sizes),
        out_shape=jax.ShapeDtypeStruct((tokens, feats), BF16),
        in_specs=[anyspace] * 6 + [vmem] + [smem] * 3 + [vmem, anyspace],
        out_specs=vmem,
        scratch_shapes=[
            pltpu.VMEM((nx, tokens + PRE, feats), BF16),
            pltpu.VMEM((depth, 4 * width + BLK), BF16),
            pltpu.VMEM((nx * width, feats), BF16),
            pltpu.VMEM((heads, BLK, 2 * BLK), F32),
            pltpu.VMEM((heads, 8, 2 * BLK), F32),
            pltpu.VMEM((heads, tokens, 2 * BLK), F32),
            pltpu.VMEM((tokens, width), F32),
            pltpu.VMEM((nx, tokens, width), BF16),
            pltpu.VMEM((BLK + 8, 2 * BLK), F32),
            pltpu.VMEM((BLK + 8, 2 * BLK), F32),
            pltpu.VMEM((ny, BLK + PRE, 2 * BLK), BF16),
            pltpu.VMEM((nz, BLK + PRE, 2 * BLK), BF16),
            pltpu.VMEM((BLK, BLK), F32),
            pltpu.VMEM((heads, BLK, BLK), F32),
            dma((7,)),
            dma((nx,)),
            dma((nx,)),
            dma((2, chunks)),
            dma((2, chunks)),
            dma((2, chunks)),
            dma((2, chunks)),
            dma((nx - 1,)),
            dma((nx - 1,)),
            dma((2,)),
            dma((2,)),
            dma((3,)),
            dma((3,)),
            dma((zc,)),
            dma((zc,)),
            dma((2, chunks)),
            dma((2, chunks)),
            dma((2, chunks)),
            dma((2, chunks)),
        ],
        compiler_params=pltpu.CompilerParams(
            collective_id=0, has_side_effects=True, vmem_limit_bytes=48 * 2**20
        ),
        name="layer",
    )(
        layer_in,
        query_weight,
        key_weight,
        value_weight,
        gate_weight,
        small,
        conv_weight,
        decay_log,
        beta_bias,
        decay_bias,
        norm_gain,
        out_weight,
    )


def solution(mesh):
    sizes = {"z": 8, "y": 4, "c": 2, "x": mesh.shape["head"]}
    finer = Mesh(
        mesh.devices.reshape(sizes["z"], sizes["y"], sizes["c"], sizes["x"]),
        ("z", "y", "c", "x"),
    )
    return jax.shard_map(
        functools.partial(on_device, sizes),
        mesh=finer,
        in_specs=(
            P(SEQ, "x"),
            P(None, "x"),
            P(None, "x"),
            P(None, "x"),
            P(None, "x"),
            P(None, "x"),
            P(None, "x"),
            P(None, None, "x"),
            P("x"),
            P("x"),
            P("x"),
            P(),
            P("x", None),
        ),
        out_specs=P(SEQ, "x"),
        check_vma=False,
    )
```

```python
import functools

import jax
import jax.numpy as jnp
from jax import lax
from jax.experimental import pallas as pl
from jax.experimental.pallas import tpu as pltpu
from jax.sharding import Mesh
from jax.sharding import PartitionSpec as P

F32 = jnp.float32
BF16 = jnp.bfloat16
MESH = pl.DeviceIdType.MESH
SEQ = ("z", "y", "c")
BLK = 128
HALF = BLK // 2
PRE = 16
PIECES = ((0, 80), (80, 64))
NORM_FLOOR = 0.0001

NN = (((1,), (0,)), ((), ()))


def dot1(a, b):
    return lax.dot_general(a, b, NN, preferred_element_type=F32)


def halves(a):
    hi = a.astype(BF16)
    lo = (a - hi.astype(F32)).astype(BF16)
    return hi, lo


def left3(a):
    hi, lo = halves(a)
    return jnp.concatenate([hi, hi, lo], axis=1)


def right3(b):
    hi, lo = halves(b)
    return jnp.concatenate([hi, lo, hi], axis=0)


def dot3(a, b):
    return dot1(left3(a), right3(b))


def dot_exact_left(a_bf16, b):
    hi, lo = halves(b)
    return dot1(
        jnp.concatenate([a_bf16, a_bf16], axis=1), jnp.concatenate([hi, lo], axis=0)
    )


def sigmoid(v):
    return 1.0 / (1.0 + jnp.exp(-v))


def silu(v):
    return v / (1.0 + jnp.exp(-v))


def softplus(v):
    return jnp.maximum(v, 0.0) + jnp.log(1.0 + jnp.exp(-jnp.abs(v)))


def compose(later, earlier):
    l2, b2, c2 = later
    l1, b1, c1 = earlier
    moved = dot3(l2, jnp.concatenate([l1, b1], axis=1))
    width = l1.shape[1]
    return (
        c2[:, :width] * l1 + c1[:, :width] * l2 - moved[:, :width],
        c2[:, :width] * b1 + b2 - moved[:, width:],
        c1 * c2,
    )


def apply_map(m, state):
    l, b, c = m
    return c[:, : state.shape[1]] * state - dot3(l, state) + b


def pick(flag, m, other):
    return jax.tree.map(lambda a, b: jnp.where(flag, a, b), m, other)


def kernel(
    sizes,
    x_in,
    wq,
    wk,
    wv,
    wg,
    wb_in,
    wd_in,
    conv_in,
    decay_log_in,
    beta_bias_in,
    decay_bias_in,
    norm_gain_in,
    w_out,
    out,
    xg,
    w_all,
    col_w,
    state,
    logsum,
    prelim,
    gate,
    hg,
    sc_send,
    sc_recv,
    yb,
    zb,
    fin_send,
    sin,
    wb,
    wd,
    conv_w,
    norm_gain,
    decay_log,
    beta_bias,
    decay_bias,
    load_sem,
    pre_send,
    pre_recv,
    d_send,
    d_recv,
    f_send,
    f_recv,
    w_send,
    w_recv,
    c_send,
    c_recv,
    y_send,
    y_recv,
    z_send,
    z_recv,
    hd_send,
    hd_recv,
    hf_send,
    hf_recv,
):
    nz, ny, nx = sizes["z"], sizes["y"], sizes["x"]
    z = lax.axis_index("z")
    y = lax.axis_index("y")
    c = lax.axis_index("c")
    x = lax.axis_index("x")
    tokens = x_in.shape[0]
    feats = x_in.shape[1]
    chunks = tokens // BLK
    heads = 2
    width = heads * BLK
    right, left = lax.rem(x + 1, nx), lax.rem(x + nx - 1, nx)
    far = lax.rem(x + 2, nx)
    count = nz * ny * 2
    here = (z * ny + y) * 2 + c
    after = lax.rem(here + 1, count)
    prior = lax.rem(here + count - 1, count)

    def place(s, xx):
        return {"z": s // (ny * 2), "y": lax.rem(s // 2, ny), "c": lax.rem(s, 2), "x": xx}

    weights = (wq, wk, wv, wg)
    loads = [pltpu.make_async_copy(x_in, xg.at[x, pl.ds(PRE, tokens), :], load_sem.at[0])]
    loads[0].start()
    for i, w in enumerate(weights):
        cp = pltpu.make_async_copy(
            w, w_all.at[:, pl.ds(i * width, width)], load_sem.at[1 + i]
        )
        cp.start()
        loads.append(cp)
    small_loads = (
        (wb_in, wb),
        (wd_in, wd),
        (conv_in, conv_w),
        (norm_gain_in, norm_gain),
        (decay_log_in, decay_log),
        (beta_bias_in, beta_bias),
        (decay_bias_in, decay_bias),
    )
    for i, (src, dst) in enumerate(small_loads):
        cp = pltpu.make_async_copy(src, dst, load_sem.at[6 + i])
        cp.start()
        loads.append(cp)
    own_cols = pltpu.make_async_copy(
        w_out.at[:, pl.ds(pl.multiple_of(x * feats, feats), feats)],
        col_w.at[pl.ds(pl.multiple_of(x * width, width), width), :],
        load_sem.at[5],
    )
    own_cols.start()

    barrier = pltpu.get_barrier_semaphore()
    up_y, down_y = lax.rem(y + 1, ny), lax.rem(y + ny - 1, ny)
    up_z, down_z = lax.rem(z + 1, nz), lax.rem(z + nz - 1, nz)
    partners = [{"x": right}, {"x": left}, {"x": far}, {"c": 1 - c}]
    partners += [{"y": up_y}, {"y": down_y}, {"z": up_z}, {"z": down_z}]
    partners += [place(after, i) for i in range(nx)]
    partners += [place(prior, i) for i in range(nx)]
    for who in partners:
        pl.semaphore_signal(barrier, inc=1, device_id=who, device_id_type=MESH)

    state[...] = jnp.zeros_like(state)
    eye = (
        lax.broadcasted_iota(jnp.int32, (BLK, BLK), 0)
        == lax.broadcasted_iota(jnp.int32, (BLK, BLK), 1)
    ).astype(F32)
    for h in range(heads):
        state[h, :, 0:BLK] = eye
    logsum[...] = jnp.zeros_like(logsum)
    pl.semaphore_wait(barrier, len(partners))
    loads[0].wait()

    def remote(src, dst, send, recv, who):
        return pltpu.make_async_remote_copy(
            src_ref=src,
            dst_ref=dst,
            send_sem=send,
            recv_sem=recv,
            device_id=who,
            device_id_type=MESH,
        )


    def ring(buf, base, send, recv, relay_send, relay_recv):
        def direct(way, t):
            rows = pl.ds(pl.multiple_of(base + t * BLK, PRE), BLK)
            return remote(
                buf.at[x, rows, :],
                buf.at[x, rows, :],
                send.at[way, t],
                recv.at[way, t],
                {"x": (right, left)[way]},
            )

        def relay(way, t):
            rows = pl.ds(pl.multiple_of(base + t * BLK + way * HALF, PRE), HALF)
            source = (left, right)[way]
            return remote(
                buf.at[source, rows, :],
                buf.at[source, rows, :],
                relay_send.at[way, t],
                relay_recv.at[way, t],
                {"x": (right, left)[way]},
            )

        return direct, relay

    direct, relay = ring(xg, PRE, d_send, d_recv, f_send, f_recv)

    def pre_copy(i):
        return remote(
            xg.at[x, pl.ds(tokens, PRE), :],
            xg.at[x, pl.ds(0, PRE), :],
            pre_send.at[i],
            pre_recv.at[x],
            place(after, i),
        )

    for i in range(nx):
        pre_copy(i).start()
    for t in range(2):
        for way in range(2):
            direct(way, t).start()
    for cp in loads[1:]:
        cp.wait()
    depth = wb.shape[1]
    wide_row = lax.broadcasted_iota(jnp.int32, (8, BLK), 0)
    for i in range(depth // BLK):
        cols = slice(i * BLK, (i + 1) * BLK)
        b_rows, d_rows = wb[:, cols].astype(F32), wd[:, cols].astype(F32)
        tile = jnp.where(wide_row == 0, b_rows[0:1], 0.0)
        tile = jnp.where(wide_row == 1, b_rows[1:2], tile)
        tile = jnp.where(wide_row == 2, d_rows[0:1], tile)
        tile = jnp.where(wide_row == 3, d_rows[1:2], tile)
        tile = jnp.concatenate([tile, jnp.zeros((BLK - 8, BLK), F32)], axis=0)
        w_all[cols, 4 * width :] = jnp.transpose(tile).astype(BF16)

    row_i = lax.broadcasted_iota(jnp.int32, (BLK, BLK), 0)
    col_i = lax.broadcasted_iota(jnp.int32, (BLK, BLK), 1)
    differ = jnp.bitwise_xor(row_i, col_i)
    within = row_i >= col_i
    before = row_i > col_i

    lane = lax.broadcasted_iota(jnp.int32, (1, BLK), 1)
    bias_row = jnp.where(lane == 0, beta_bias[0], 0.0)
    bias_row = jnp.where(lane == 1, beta_bias[1], bias_row)
    bias_row = jnp.where(lane == 2, decay_bias[0], bias_row)
    bias_row = jnp.where(lane == 3, decay_bias[1], bias_row)
    rate_row = jnp.where(lane == 2, decay_log[0], -200.0)
    rate_row = jnp.exp(jnp.where(lane == 3, decay_log[1], rate_row))
    gain_row = norm_gain[...].reshape(1, BLK)

    def unit_rows(v):
        return v * lax.rsqrt(jnp.sum(v * v, axis=-1, keepdims=True) + 1.0)

    def chunk(t):
        start = pl.multiple_of(t * BLK, BLK)
        rows = pl.ds(start, BLK + PRE)
        xs = jnp.concatenate([xg[p, rows, :] for p in range(nx)], axis=1)
        first = jnp.logical_and(here == 0, t == 0)
        ext_row = lax.broadcasted_iota(jnp.int32, (BLK + PRE, 3 * width), 0)
        raw = dot1(xs, w_all[...])
        qkv = raw[:, 0 : 3 * width]
        qkv = jnp.where(jnp.logical_and(first, ext_row < PRE), 0.0, qkv)
        taps = [
            jnp.concatenate([conv_w[i, s : s + 1, :] for i in range(3)], axis=1)
            for s in range(4)
        ]
        mixed = taps[0] * qkv
        for s in range(1, 4):
            mixed = mixed + taps[s] * pltpu.roll(qkv, s, 0)
        mixed = silu(mixed[PRE:])
        out_rows = pl.ds(start, BLK)
        gates = silu(raw[PRE:, 3 * width : 4 * width])
        for h in range(heads):
            gate[out_rows, h * BLK : (h + 1) * BLK] = (
                gates[:, h * BLK : (h + 1) * BLK] * gain_row
            )
        small = raw[PRE:, 4 * width :] + bias_row
        betas = sigmoid(small)
        steps = -rate_row * softplus(small)
        s_hi = steps.astype(BF16)
        rest = steps - s_hi.astype(F32)
        s_mid = rest.astype(BF16)
        s_lo = (rest - s_mid.astype(F32)).astype(BF16)
        tri = within.astype(F32).astype(BF16)
        total = dot1(
            jnp.concatenate([tri, tri, tri], axis=1),
            jnp.concatenate([s_hi, s_mid, s_lo], axis=0),
        )
        total_t = jnp.transpose(total)
        both = []
        for h in range(heads):
            cols = slice(h * BLK, (h + 1) * BLK)
            q = unit_rows(mixed[:, h * BLK : (h + 1) * BLK])
            k = unit_rows(mixed[:, width + h * BLK : width + (h + 1) * BLK])
            v = mixed[:, 2 * width + h * BLK : 2 * width + (h + 1) * BLK]
            beta = betas[:, h : h + 1]
            run_c = total[:, 2 + h : 3 + h]
            run_r = total_t[2 + h : 3 + h, :]
            end = run_r[:, BLK - 1 : BLK]
            decay = jnp.where(within, jnp.exp(jnp.minimum(run_c - run_r, 0.0)), 0.0)
            kt = jnp.transpose(k)
            scores = dot3(jnp.concatenate([k, q], axis=0), kt)
            low = jnp.where(before, beta * decay * scores[:BLK], 0.0)
            mix = decay * scores[BLK:]
            grow = jnp.exp(run_c)
            ext = state[h]
            read = dot3(
                jnp.concatenate([(beta * grow) * k, grow * q], axis=0), ext
            )
            right_side = (
                jnp.concatenate([jnp.zeros_like(v), beta * v], axis=1) - read[:BLK]
            )
            both.append((low, mix, right_side, read[BLK:], kt, run_r, end, ext))
        first_links = [jnp.where(differ == 1, b[0], 0.0) for b in both]
        inv = [jnp.where(row_i == col_i, 1.0, 0.0) - m for m in first_links]
        rest = []
        for b, m in zip(both, first_links):
            later = jnp.where(differ > 1, b[0], 0.0)
            rest.append(later - dot3(later, m))
        w = 2
        while w < BLK:
            linking = jnp.logical_and(differ >= w, differ < 2 * w)
            links = [right3(jnp.where(linking, r, 0.0)) for r in rest]
            if 2 * w < BLK:
                later = [jnp.where(differ >= 2 * w, r, 0.0) for r in rest]
                stacked = [
                    jnp.concatenate([r, a], axis=0) for r, a in zip(later, inv)
                ]
                moved = [s - dot1(left3(s), m) for s, m in zip(stacked, links)]
                rest = [m[:BLK] for m in moved]
                inv = [m[BLK:] for m in moved]
            else:
                inv = [a - dot1(left3(a), m) for a, m in zip(inv, links)]
            w *= 2
        for h in range(heads):
            low, mix, right_side, carried, kt, run_r, end, ext = both[h]
            solved = dot3(inv[h], right_side)
            solved3 = right3(solved)
            prelim[h, out_rows, :] = carried + dot1(left3(mix), solved3)
            weighted = kt * jnp.exp(end - run_r)
            state[h] = jnp.exp(end) * ext + dot1(left3(weighted), solved3)
            logsum[h] = logsum[h] + jnp.broadcast_to(end, logsum.shape[1:])

    def step(t, carry):
        @pl.when(t < chunks)
        def _():
            direct(0, t).wait_recv()
            direct(1, t).wait_recv()
            relay(0, t).start()
            relay(1, t).start()

        @pl.when(t < chunks - 2)
        def _():
            direct(0, t + 2).start()
            direct(1, t + 2).start()

        @pl.when(t == 0)
        def _():
            for i in range(nx):
                remote(
                    xg.at[i, pl.ds(tokens, PRE), :],
                    xg.at[i, pl.ds(0, PRE), :],
                    pre_send.at[i],
                    pre_recv.at[i],
                    place(after, i),
                ).wait_recv()

        @pl.when(t > 0)
        def _():
            relay(0, t - 1).wait_recv()
            relay(1, t - 1).wait_recv()
            chunk(t - 1)

        return carry

    lax.fori_loop(0, chunks + 1, step, 0)

    def columns(j):
        who = lax.rem(x + j, nx)
        return remote(
            w_out.at[:, pl.ds(pl.multiple_of(who * feats, feats), feats)],
            col_w.at[pl.ds(pl.multiple_of(x * width, width), width), :],
            w_send.at[j - 1],
            w_recv.at[j - 1],
            {"x": who},
        )

    for j in range(1, nx):
        columns(j).start()

    def own_map(h):
        ext = state[h]
        keep = jnp.exp(logsum[h, 0:1, :])
        return (keep[:, :BLK] * eye - ext[:, :BLK], ext[:, BLK:], keep)

    swap = remote(sc_send, sc_recv, c_send.at[0], c_recv.at[0], {"c": 1 - c})
    give = remote(fin_send, sin, c_send.at[1], c_recv.at[1], {"c": 1 - c})

    @pl.when(c == 0)
    def _():
        for h in range(heads):
            l, b, keep = own_map(h)
            sc_send[h, 0:BLK, 0:BLK] = l
            sc_send[h, 0:BLK, BLK:] = b
            sc_send[h, BLK:, :] = jnp.broadcast_to(keep, (8, 2 * BLK))
        swap.start()
        swap.wait_send()
        give.wait_recv()

    zero = jnp.zeros((BLK, BLK), F32)
    one_row = jnp.ones((1, 2 * BLK), F32)
    identity = (zero, zero, one_row)
    each = range(heads)

    def put(buf, slot, m, h):
        l, b, keep = m
        buf[slot, h, 0:BLK, 0:BLK] = l.astype(BF16)
        buf[slot, h, 0:BLK, BLK:] = b.astype(BF16)
        hi, lo = halves(keep)
        tail = lax.broadcasted_iota(jnp.int32, (PRE, 2 * BLK), 0)
        buf[slot, h, BLK:, :] = jnp.where(
            tail == 0,
            jnp.broadcast_to(hi.astype(F32), (PRE, 2 * BLK)),
            jnp.broadcast_to(lo.astype(F32), (PRE, 2 * BLK)),
        ).astype(BF16)

    def get(buf, slot, h):
        tail = buf[slot, h, BLK:, :].astype(F32)
        return (
            buf[slot, h, 0:BLK, 0:BLK].astype(F32),
            buf[slot, h, 0:BLK, BLK:].astype(F32),
            tail[0:1] + tail[1:2],
        )

    def pieces(buf, slot, send, recv, j, who):
        made = []
        for h in each:
            for p, (at, rows) in enumerate(PIECES):
                made.append(
                    remote(
                        buf.at[slot, h, pl.ds(at, rows), :],
                        buf.at[slot, h, pl.ds(at, rows), :],
                        send.at[j, h, p],
                        recv.at[j, h, p],
                        who,
                    )
                )
        return made

    @pl.when(c == 1)
    def _():
        own = [own_map(h) for h in each]
        swap.wait_recv()
        map0 = [
            (sc_recv[h, 0:BLK, 0:BLK], sc_recv[h, 0:BLK, BLK:], sc_recv[h, BLK : BLK + 1, :])
            for h in each
        ]
        for h in each:
            put(yb, y, compose(own[h], map0[h]), h)

        y1 = pieces(yb, y, y_send, y_recv, 0, {"y": up_y})
        y2 = pieces(yb, y, y_send, y_recv, 1, {"y": down_y})
        y3 = pieces(yb, down_y, y_send, y_recv, 2, {"y": up_y})
        for a, b in zip(y1, y2):
            a.start()
            b.start()
        for a, b in zip(y1, y3):
            a.wait_recv()
            b.start()
        for b in y2:
            b.wait_recv()
        for b in y3:
            b.wait_recv()
        before_row = []
        for h in each:
            maps = [get(yb, j, h) for j in range(ny)]
            run = maps[0]
            prefix = pick(y == 0, identity, run)
            for j in range(1, ny):
                if j > 1:
                    prefix = pick(y == j, run, prefix)
                run = compose(maps[j], run)
            before_row.append(prefix)
            put(zb, z, run, h)

        ups, downs = nz // 2, nz - 1 - nz // 2
        up = [
            pieces(zb, lax.rem(z + nz - j, nz), z_send, z_recv, j, {"z": up_z})
            for j in range(ups)
        ]
        dn = [
            pieces(zb, lax.rem(z + j, nz), z_send, z_recv, ups + j, {"z": down_z})
            for j in range(downs)
        ]
        near = [identity] * heads
        low_state = [zero] * heads
        for a, b in zip(up[0], dn[0]):
            a.start()
            b.start()
        for j in range(ups):
            for p in range(len(up[0])):
                up[j][p].wait_recv()
                if j + 1 < ups:
                    up[j + 1][p].start()
                if j < downs:
                    dn[j][p].wait_recv()
                    if j + 1 < downs:
                        dn[j + 1][p].start()
            d = j + 1
            for h in each:
                got = pick(z - d >= 0, get(zb, lax.rem(z + nz - d, nz), h), identity)
                if d < ups:
                    near[h] = compose(near[h], got)
                    got = pick(z + d - nz >= 0, get(zb, lax.rem(z + d, nz), h), identity)
                    low_state[h] = apply_map(got, low_state[h])
                else:
                    row_state = apply_map(near[h], apply_map(got, low_state[h]))
                    chip_state = apply_map(before_row[h], row_state)
                    sin[h] = apply_map(map0[h], chip_state)
                    fin_send[h] = chip_state
        give.start()
        give.wait_send()
        for group in [y1, y2, y3] + up + dn:
            for a in group:
                a.wait_send()

    h_direct, h_relay = ring(hg, 0, hd_send, hd_recv, hf_send, hf_recv)
    starts = [right3(sin[h]) for h in range(heads)]
    for t in range(chunks):
        rows = slice(t * BLK, (t + 1) * BLK)
        for h in range(heads):
            part = prelim[h, rows, :]
            head_out = dot1(left3(part[:, :BLK]), starts[h]) + part[:, BLK:]
            scaled = head_out * lax.rsqrt(
                jnp.mean(head_out * head_out, axis=-1, keepdims=True) + NORM_FLOOR
            )
            cols = slice(h * BLK, (h + 1) * BLK)
            hg[x, rows, cols] = (scaled * gate[rows, cols]).astype(BF16)
        for way in range(2):
            h_direct(way, t).start()
    for t in range(chunks):
        for way in range(2):
            h_direct(way, t).wait_recv()
            h_relay(way, t).start()
    own_cols.wait()
    for j in range(1, nx):
        columns(j).wait_recv()
    for t in range(chunks):
        rows = slice(t * BLK, (t + 1) * BLK)
        for way in range(2):
            h_relay(way, t).wait_recv()
        rows_all = jnp.concatenate([hg[p, rows, :] for p in range(nx)], axis=1)
        out[rows, :] = dot1(rows_all, col_w[...]).astype(BF16)

    for i in range(nx):
        pre_copy(i).wait_send()
    for t in range(chunks):
        for way in range(2):
            direct(way, t).wait_send()
            relay(way, t).wait_send()
            h_direct(way, t).wait_send()
            h_relay(way, t).wait_send()
    for j in range(1, nx):
        columns(j).wait_send()


def on_device(
    sizes,
    layer_in,
    query_weight,
    key_weight,
    value_weight,
    gate_weight,
    beta_weight,
    decay_weight,
    conv_weight,
    decay_log,
    beta_bias,
    decay_bias,
    norm_gain,
    out_weight,
):
    tokens, feats = layer_in.shape
    depth, width = query_weight.shape
    nz, ny, nx = sizes["z"], sizes["y"], sizes["x"]
    chunks = tokens // BLK
    heads = 2
    hbm = pl.BlockSpec(memory_space=pltpu.HBM)
    vmem = pl.BlockSpec(memory_space=pltpu.VMEM)
    dma = pltpu.SemaphoreType.DMA
    zc = nz - 1
    return pl.pallas_call(
        functools.partial(kernel, sizes),
        out_shape=jax.ShapeDtypeStruct((tokens, feats), BF16),
        in_specs=[hbm] * 13,
        out_specs=vmem,
        scratch_shapes=[
            pltpu.VMEM((nx, tokens + PRE, feats), BF16),
            pltpu.VMEM((depth, 4 * width + BLK), BF16),
            pltpu.VMEM((nx * width, feats), BF16),
            pltpu.VMEM((heads, BLK, 2 * BLK), F32),
            pltpu.VMEM((heads, 8, 2 * BLK), F32),
            pltpu.VMEM((heads, tokens, 2 * BLK), F32),
            pltpu.VMEM((tokens, width), F32),
            pltpu.VMEM((nx, tokens, width), BF16),
            pltpu.VMEM((heads, BLK + 8, 2 * BLK), F32),
            pltpu.VMEM((heads, BLK + 8, 2 * BLK), F32),
            pltpu.VMEM((ny, heads, BLK + PRE, 2 * BLK), BF16),
            pltpu.VMEM((nz, heads, BLK + PRE, 2 * BLK), BF16),
            pltpu.VMEM((heads, BLK, BLK), F32),
            pltpu.VMEM((heads, BLK, BLK), F32),
            pltpu.VMEM((heads, depth), BF16),
            pltpu.VMEM((heads, depth), BF16),
            pltpu.VMEM((3, 4, width), F32),
            pltpu.VMEM((BLK,), F32),
            pltpu.SMEM((heads,), F32),
            pltpu.SMEM((heads,), F32),
            pltpu.SMEM((heads,), F32),
            dma((13,)),
            dma((nx,)),
            dma((nx,)),
            dma((2, chunks)),
            dma((2, chunks)),
            dma((2, chunks)),
            dma((2, chunks)),
            dma((nx - 1,)),
            dma((nx - 1,)),
            dma((2,)),
            dma((2,)),
            dma((3, heads, len(PIECES))),
            dma((3, heads, len(PIECES))),
            dma((zc, heads, len(PIECES))),
            dma((zc, heads, len(PIECES))),
            dma((2, chunks)),
            dma((2, chunks)),
            dma((2, chunks)),
            dma((2, chunks)),
        ],
        compiler_params=pltpu.CompilerParams(
            collective_id=0, has_side_effects=True, vmem_limit_bytes=66519040
        ),
        name="layer",
    )(
        layer_in,
        query_weight,
        key_weight,
        value_weight,
        gate_weight,
        beta_weight.T,
        decay_weight.T,
        conv_weight.transpose(1, 0, 2),
        decay_log,
        beta_bias,
        decay_bias,
        norm_gain,
        out_weight,
    )


def solution(mesh):
    sizes = {"z": 8, "y": 4, "c": 2, "x": mesh.shape["head"]}
    finer = Mesh(
        mesh.devices.reshape(sizes["z"], sizes["y"], sizes["c"], sizes["x"]),
        ("z", "y", "c", "x"),
    )
    return jax.shard_map(
        functools.partial(on_device, sizes),
        mesh=finer,
        in_specs=(
            P(SEQ, "x"),
            P(None, "x"),
            P(None, "x"),
            P(None, "x"),
            P(None, "x"),
            P(None, "x"),
            P(None, "x"),
            P(None, None, "x"),
            P("x"),
            P("x"),
            P("x"),
            P(),
            P("x", None),
        ),
        out_specs=P(SEQ, "x"),
        check_vma=False,
    )
```

```python
import functools

import jax
import jax.numpy as jnp
from jax import lax
from jax.experimental import pallas as pl
from jax.experimental.pallas import tpu as pltpu
from jax.sharding import Mesh
from jax.sharding import PartitionSpec as P

F32 = jnp.float32
BF16 = jnp.bfloat16
MESH = pl.DeviceIdType.MESH
SEQ = ("z", "y", "c")
BLK = 128
HALF = BLK // 2
PRE = 16
SENT = 8
PIECES = ((0, 80), (80, 64))
NORM_FLOOR = 0.0001

NN = (((1,), (0,)), ((), ()))


def dot1(a, b):
    return lax.dot_general(a, b, NN, preferred_element_type=F32)


def halves(a):
    hi = a.astype(BF16)
    lo = (a - hi.astype(F32)).astype(BF16)
    return hi, lo


def left3(a):
    hi, lo = halves(a)
    return jnp.concatenate([hi, hi, lo], axis=1)


def right3(b):
    hi, lo = halves(b)
    return jnp.concatenate([hi, lo, hi], axis=0)


def dot3(a, b):
    return dot1(left3(a), right3(b))


def product(a, b, exact_a=False, exact_b=False):
    if exact_a and exact_b:
        return dot1(a.astype(BF16), b.astype(BF16))
    if exact_a:
        hi, lo = halves(b)
        a = a.astype(BF16)
        return dot1(jnp.concatenate([a, a], axis=1), jnp.concatenate([hi, lo], axis=0))
    if exact_b:
        hi, lo = halves(a)
        b = b.astype(BF16)
        return dot1(jnp.concatenate([hi, lo], axis=1), jnp.concatenate([b, b], axis=0))
    return dot3(a, b)


def sigmoid(v):
    return 1.0 / (1.0 + jnp.exp(-v))


def silu(v):
    return v / (1.0 + jnp.exp(-v))


def softplus(v):
    return jnp.maximum(v, 0.0) + jnp.log(1.0 + jnp.exp(-jnp.abs(v)))


def compose(later, earlier, *exact):
    l2, b2, c2 = later
    l1, b1, c1 = earlier
    moved = product(l2, jnp.concatenate([l1, b1], axis=1), *exact)
    width = l1.shape[1]
    return (
        c2[:, :width] * l1 + c1[:, :width] * l2 - moved[:, :width],
        c2[:, :width] * b1 + b2 - moved[:, width:],
        c1 * c2,
    )


def apply_map(m, state, *exact):
    l, b, c = m
    return c[:, : state.shape[1]] * state - product(l, state, *exact) + b


def pick(flag, m, other):
    return jax.tree.map(lambda a, b: jnp.where(flag, a, b), m, other)


def kernel(
    sizes,
    x_in,
    wq,
    wk,
    wv,
    wg,
    wb_in,
    wd_in,
    conv_in,
    decay_log_in,
    beta_bias_in,
    decay_bias_in,
    norm_gain_in,
    w_out,
    out,
    xg,
    w_all,
    col_w,
    state,
    logsum,
    prelim,
    gate,
    hg,
    sc_send,
    sc_recv,
    yb,
    zb,
    fin_send,
    sin,
    wb,
    wd,
    conv_w,
    norm_gain,
    decay_log,
    beta_bias,
    decay_bias,
    load_sem,
    pre_send,
    pre_recv,
    d_send,
    d_recv,
    f_send,
    f_recv,
    w_send,
    w_recv,
    hand_send,
    hand_recv,
    c_send,
    c_recv,
    y_send,
    y_recv,
    z_send,
    z_recv,
    hd_send,
    hd_recv,
    hf_send,
    hf_recv,
):
    nz, ny, nx = sizes["z"], sizes["y"], sizes["x"]
    z = lax.axis_index("z")
    y = lax.axis_index("y")
    c = lax.axis_index("c")
    x = lax.axis_index("x")
    tokens = x_in.shape[0]
    feats = x_in.shape[1]
    chunks = tokens // BLK
    heads = 2
    width = heads * BLK
    right, left = lax.rem(x + 1, nx), lax.rem(x + nx - 1, nx)
    far = lax.rem(x + 2, nx)
    count = nz * ny * 2
    here = (z * ny + y) * 2 + c
    after = lax.rem(here + 1, count)
    prior = lax.rem(here + count - 1, count)

    def place(s, xx):
        return {"z": s // (ny * 2), "y": lax.rem(s // 2, ny), "c": lax.rem(s, 2), "x": xx}

    xg[:, 0:PRE, :] = jnp.zeros((nx, PRE, feats), BF16)

    weights = (wq, wk, wv, wg)
    loads = [pltpu.make_async_copy(x_in, xg.at[x, pl.ds(PRE, tokens), :], load_sem.at[0])]
    loads[0].start()
    for i, w in enumerate(weights):
        cp = pltpu.make_async_copy(
            w, w_all.at[:, pl.ds(i * width, width)], load_sem.at[1 + i]
        )
        cp.start()
        loads.append(cp)
    small_loads = (
        (wb_in, wb),
        (wd_in, wd),
        (conv_in, conv_w),
        (norm_gain_in, norm_gain),
        (decay_log_in, decay_log),
        (beta_bias_in, beta_bias),
        (decay_bias_in, decay_bias),
    )
    for i, (src, dst) in enumerate(small_loads):
        cp = pltpu.make_async_copy(src, dst, load_sem.at[6 + i])
        cp.start()
        loads.append(cp)
    own_cols = pltpu.make_async_copy(
        w_out.at[:, pl.ds(pl.multiple_of(x * feats, feats), feats)],
        col_w.at[pl.ds(pl.multiple_of(x * width, width), width), :],
        load_sem.at[5],
    )
    own_cols.start()

    barrier = pltpu.get_barrier_semaphore()
    up_y, down_y = lax.rem(y + 1, ny), lax.rem(y + ny - 1, ny)
    up_z, down_z = lax.rem(z + 1, nz), lax.rem(z + nz - 1, nz)
    partners = [{"x": right}, {"x": left}, {"x": far}, {"c": 1 - c}]
    partners += [{"y": up_y}, {"y": down_y}, {"z": up_z}, {"z": down_z}]
    partners += [place(after, i) for i in range(nx)]
    partners += [place(prior, i) for i in range(nx)]
    for who in partners:
        pl.semaphore_signal(barrier, inc=1, device_id=who, device_id_type=MESH)

    state[...] = jnp.zeros_like(state)
    eye = (
        lax.broadcasted_iota(jnp.int32, (BLK, BLK), 0)
        == lax.broadcasted_iota(jnp.int32, (BLK, BLK), 1)
    ).astype(F32)
    for h in range(heads):
        state[h, :, 0:BLK] = eye
    logsum[...] = jnp.zeros_like(logsum)
    pl.semaphore_wait(barrier, len(partners))
    loads[0].wait()

    def remote(src, dst, send, recv, who):
        return pltpu.make_async_remote_copy(
            src_ref=src,
            dst_ref=dst,
            send_sem=send,
            recv_sem=recv,
            device_id=who,
            device_id_type=MESH,
        )


    def ring(buf, base, send, recv, relay_send, relay_recv):
        def direct(way, t):
            rows = pl.ds(pl.multiple_of(base + t * BLK, PRE), BLK)
            return remote(
                buf.at[x, rows, :],
                buf.at[x, rows, :],
                send.at[way, t],
                recv.at[way, t],
                {"x": (right, left)[way]},
            )

        def relay(way, t):
            rows = pl.ds(pl.multiple_of(base + t * BLK + way * HALF, PRE), HALF)
            source = (left, right)[way]
            return remote(
                buf.at[source, rows, :],
                buf.at[source, rows, :],
                relay_send.at[way, t],
                relay_recv.at[way, t],
                {"x": (right, left)[way]},
            )

        return direct, relay

    direct, relay = ring(xg, PRE, d_send, d_recv, f_send, f_recv)

    def pre_copy(i):
        return remote(
            xg.at[x, pl.ds(tokens + SENT, SENT), :],
            xg.at[x, pl.ds(SENT, SENT), :],
            pre_send.at[i],
            pre_recv.at[x],
            place(after, i),
        )

    for i in range(nx):
        pre_copy(i).start()
    for t in range(2):
        for way in range(2):
            direct(way, t).start()
    for cp in loads[1:]:
        cp.wait()
    depth = wb.shape[1]
    wide_row = lax.broadcasted_iota(jnp.int32, (8, BLK), 0)
    for i in range(depth // BLK):
        cols = slice(i * BLK, (i + 1) * BLK)
        b_rows, d_rows = wb[:, cols].astype(F32), wd[:, cols].astype(F32)
        tile = jnp.where(wide_row == 0, b_rows[0:1], 0.0)
        tile = jnp.where(wide_row == 1, b_rows[1:2], tile)
        tile = jnp.where(wide_row == 2, d_rows[0:1], tile)
        tile = jnp.where(wide_row == 3, d_rows[1:2], tile)
        tile = jnp.concatenate([tile, jnp.zeros((BLK - 8, BLK), F32)], axis=0)
        w_all[cols, 4 * width :] = jnp.transpose(tile).astype(BF16)

    row_i = lax.broadcasted_iota(jnp.int32, (BLK, BLK), 0)
    col_i = lax.broadcasted_iota(jnp.int32, (BLK, BLK), 1)
    differ = jnp.bitwise_xor(row_i, col_i)
    within = row_i >= col_i
    before = row_i > col_i

    lane = lax.broadcasted_iota(jnp.int32, (1, BLK), 1)
    bias_row = jnp.where(lane == 0, beta_bias[0], 0.0)
    bias_row = jnp.where(lane == 1, beta_bias[1], bias_row)
    bias_row = jnp.where(lane == 2, decay_bias[0], bias_row)
    bias_row = jnp.where(lane == 3, decay_bias[1], bias_row)
    rate_row = jnp.where(lane == 2, decay_log[0], -200.0)
    rate_row = jnp.exp(jnp.where(lane == 3, decay_log[1], rate_row))
    gain_row = norm_gain[...].reshape(1, BLK)

    def unit_rows(v):
        return v * lax.rsqrt(jnp.sum(v * v, axis=-1, keepdims=True) + 1.0)

    def chunk(t):
        start = pl.multiple_of(t * BLK, BLK)
        rows = pl.ds(start, BLK + PRE)
        xs = jnp.concatenate([xg[p, rows, :] for p in range(nx)], axis=1)
        first = jnp.logical_and(here == 0, t == 0)
        ext_row = lax.broadcasted_iota(jnp.int32, (BLK + PRE, 3 * width), 0)
        raw = dot1(xs, w_all[...])
        qkv = raw[:, 0 : 3 * width]
        qkv = jnp.where(jnp.logical_and(first, ext_row < PRE), 0.0, qkv)
        taps = [
            jnp.concatenate([conv_w[i, s : s + 1, :] for i in range(3)], axis=1)
            for s in range(4)
        ]
        mixed = taps[0] * qkv
        for s in range(1, 4):
            mixed = mixed + taps[s] * pltpu.roll(qkv, s, 0)
        mixed = silu(mixed[PRE:])
        out_rows = pl.ds(start, BLK)
        gates = silu(raw[PRE:, 3 * width : 4 * width])
        for h in range(heads):
            gate[out_rows, h * BLK : (h + 1) * BLK] = (
                gates[:, h * BLK : (h + 1) * BLK] * gain_row
            )
        small = raw[PRE:, 4 * width :] + bias_row
        betas = sigmoid(small)
        steps = -rate_row * softplus(small)
        s_hi = steps.astype(BF16)
        rest = steps - s_hi.astype(F32)
        s_mid = rest.astype(BF16)
        s_lo = (rest - s_mid.astype(F32)).astype(BF16)
        tri = within.astype(F32).astype(BF16)
        total = dot1(
            jnp.concatenate([tri, tri, tri], axis=1),
            jnp.concatenate([s_hi, s_mid, s_lo], axis=0),
        )
        total_t = jnp.transpose(total)
        both = []
        for h in range(heads):
            cols = slice(h * BLK, (h + 1) * BLK)
            q = unit_rows(mixed[:, h * BLK : (h + 1) * BLK])
            k = unit_rows(mixed[:, width + h * BLK : width + (h + 1) * BLK])
            v = mixed[:, 2 * width + h * BLK : 2 * width + (h + 1) * BLK]
            beta = betas[:, h : h + 1]
            run_c = total[:, 2 + h : 3 + h]
            run_r = total_t[2 + h : 3 + h, :]
            end = run_r[:, BLK - 1 : BLK]
            decay = jnp.where(within, jnp.exp(jnp.minimum(run_c - run_r, 0.0)), 0.0)
            kt = jnp.transpose(k)
            scores = dot3(jnp.concatenate([k, q], axis=0), kt)
            low = jnp.where(before, beta * decay * scores[:BLK], 0.0)
            mix = decay * scores[BLK:]
            grow = jnp.exp(run_c)
            ext = state[h]
            read = dot3(
                jnp.concatenate([(beta * grow) * k, grow * q], axis=0), ext
            )
            right_side = (
                jnp.concatenate([jnp.zeros_like(v), beta * v], axis=1) - read[:BLK]
            )
            both.append((low, mix, right_side, read[BLK:], kt, run_r, end, ext))
        first_links = [jnp.where(differ == 1, b[0], 0.0) for b in both]
        inv = [jnp.where(row_i == col_i, 1.0, 0.0) - m for m in first_links]
        rest = []
        for b, m in zip(both, first_links):
            later = jnp.where(differ > 1, b[0], 0.0)
            rest.append(later - dot3(later, m))
        w = 2
        while w < BLK:
            linking = jnp.logical_and(differ >= w, differ < 2 * w)
            links = [right3(jnp.where(linking, r, 0.0)) for r in rest]
            if 2 * w < BLK:
                later = [jnp.where(differ >= 2 * w, r, 0.0) for r in rest]
                stacked = [
                    jnp.concatenate([r, a], axis=0) for r, a in zip(later, inv)
                ]
                moved = [s - dot1(left3(s), m) for s, m in zip(stacked, links)]
                rest = [m[:BLK] for m in moved]
                inv = [m[BLK:] for m in moved]
            else:
                inv = [a - dot1(left3(a), m) for a, m in zip(inv, links)]
            w *= 2
        for h in range(heads):
            low, mix, right_side, carried, kt, run_r, end, ext = both[h]
            solved = dot3(inv[h], right_side)
            solved3 = right3(solved)
            prelim[h, out_rows, :] = carried + dot1(left3(mix), solved3)
            weighted = kt * jnp.exp(end - run_r)
            state[h] = jnp.exp(end) * ext + dot1(left3(weighted), solved3)
            logsum[h] = logsum[h] + jnp.broadcast_to(end, logsum.shape[1:])

    def step(t, carry):
        @pl.when(t < chunks)
        def _():
            direct(0, t).wait_recv()
            direct(1, t).wait_recv()
            relay(0, t).start()
            relay(1, t).start()

        @pl.when(t < chunks - 2)
        def _():
            direct(0, t + 2).start()
            direct(1, t + 2).start()

        @pl.when(t == 0)
        def _():
            for i in range(nx):
                remote(
                    xg.at[i, pl.ds(tokens + SENT, SENT), :],
                    xg.at[i, pl.ds(SENT, SENT), :],
                    pre_send.at[i],
                    pre_recv.at[i],
                    place(after, i),
                ).wait_recv()

        @pl.when(t > 0)
        def _():
            relay(0, t - 1).wait_recv()
            relay(1, t - 1).wait_recv()
            chunk(t - 1)

        return carry

    lax.fori_loop(0, chunks + 1, step, 0)

    def columns(j):
        who = lax.rem(x + j, nx)
        return remote(
            w_out.at[:, pl.ds(pl.multiple_of(who * feats, feats), feats)],
            col_w.at[pl.ds(pl.multiple_of(x * width, width), width), :],
            w_send.at[j - 1],
            w_recv.at[j - 1],
            {"x": who},
        )

    def handed(j):
        rows = pl.ds(pl.multiple_of(lax.rem(x + nx - j, nx) * width, width), width)
        return remote(
            col_w.at[rows, :],
            col_w.at[rows, :],
            hand_send.at[j - 1],
            hand_recv.at[j - 1],
            {"c": 1 - c},
        )

    @pl.when(c == 0)
    def _():
        for j in range(1, nx):
            columns(j).start()


    def own_map(h):
        ext = state[h]
        keep = jnp.exp(logsum[h, 0:1, :])
        return (keep[:, :BLK] * eye - ext[:, :BLK], ext[:, BLK:], keep)

    swap = remote(sc_send, sc_recv, c_send.at[0], c_recv.at[0], {"c": 1 - c})
    give = remote(fin_send, sin, c_send.at[1], c_recv.at[1], {"c": 1 - c})

    @pl.when(c == 0)
    def _():
        for h in range(heads):
            l, b, keep = own_map(h)
            sc_send[h, 0:BLK, 0:BLK] = l
            sc_send[h, 0:BLK, BLK:] = b
            sc_send[h, BLK:, :] = jnp.broadcast_to(keep, (8, 2 * BLK))
        swap.start()
        swap.wait_send()
        for j in range(1, nx):
            columns(j).wait_recv()
            handed(j).start()
        for j in range(1, nx):
            columns(j).wait_send()
            handed(j).wait_send()
        give.wait_recv()

    zero = jnp.zeros((BLK, BLK), F32)
    one_row = jnp.ones((1, 2 * BLK), F32)
    identity = (zero, zero, one_row)
    each = range(heads)

    def put(buf, slot, m, h):
        l, b, keep = m
        buf[slot, h, 0:BLK, 0:BLK] = l.astype(BF16)
        buf[slot, h, 0:BLK, BLK:] = b.astype(BF16)
        hi, lo = halves(keep)
        tail = lax.broadcasted_iota(jnp.int32, (PRE, 2 * BLK), 0)
        buf[slot, h, BLK:, :] = jnp.where(
            tail == 0,
            jnp.broadcast_to(hi.astype(F32), (PRE, 2 * BLK)),
            jnp.broadcast_to(lo.astype(F32), (PRE, 2 * BLK)),
        ).astype(BF16)

    def get(buf, slot, h):
        tail = buf[slot, h, BLK:, :].astype(F32)
        return (
            buf[slot, h, 0:BLK, 0:BLK].astype(F32),
            buf[slot, h, 0:BLK, BLK:].astype(F32),
            tail[0:1] + tail[1:2],
        )

    def pieces(buf, slot, send, recv, j, who):
        made = []
        for h in each:
            for p, (at, rows) in enumerate(PIECES):
                made.append(
                    remote(
                        buf.at[slot, h, pl.ds(at, rows), :],
                        buf.at[slot, h, pl.ds(at, rows), :],
                        send.at[j, h, p],
                        recv.at[j, h, p],
                        who,
                    )
                )
        return made

    @pl.when(c == 1)
    def _():
        own = [own_map(h) for h in each]
        swap.wait_recv()
        map0 = [
            (sc_recv[h, 0:BLK, 0:BLK], sc_recv[h, 0:BLK, BLK:], sc_recv[h, BLK : BLK + 1, :])
            for h in each
        ]
        for h in each:
            put(yb, y, compose(own[h], map0[h]), h)

        y1 = pieces(yb, y, y_send, y_recv, 0, {"y": up_y})
        y2 = pieces(yb, y, y_send, y_recv, 1, {"y": down_y})
        y3 = pieces(yb, down_y, y_send, y_recv, 2, {"y": up_y})
        for a, b in zip(y1, y2):
            a.start()
            b.start()
        for a, b in zip(y1, y3):
            a.wait_recv()
            b.start()
        for b in y2:
            b.wait_recv()
        for b in y3:
            b.wait_recv()
        before_row = []
        for h in each:
            maps = [get(yb, j, h) for j in range(ny)]
            low_pair = compose(maps[1], maps[0], True, True)
            high_pair = compose(maps[3], maps[2], True, True)
            triple = compose(maps[2], low_pair, True)
            run = compose(high_pair, low_pair)
            prefix = pick(y == 0, identity, maps[0])
            prefix = pick(y == 2, low_pair, prefix)
            prefix = pick(y == 3, triple, prefix)
            before_row.append(prefix)
            put(zb, z, run, h)

        ups, downs = nz // 2, nz - 1 - nz // 2
        up = [
            pieces(zb, lax.rem(z + nz - j, nz), z_send, z_recv, j, {"z": up_z})
            for j in range(ups)
        ]
        dn = [
            pieces(zb, lax.rem(z + j, nz), z_send, z_recv, ups + j, {"z": down_z})
            for j in range(downs)
        ]
        near = [identity] * heads
        low_state = [zero] * heads
        own_near = [identity] * heads
        for a, b in zip(up[0], dn[0]):
            a.start()
            b.start()
        for j in range(ups):
            for p in range(len(up[0])):
                up[j][p].wait_recv()
                if j + 1 < ups:
                    up[j + 1][p].start()
                if j < downs:
                    dn[j][p].wait_recv()
                    if j + 1 < downs:
                        dn[j + 1][p].start()
            d = j + 1
            for h in each:
                got = pick(z - d >= 0, get(zb, lax.rem(z + nz - d, nz), h), identity)
                if d < ups:
                    near[h] = compose(near[h], got, False, True)
                    got = pick(z + d - nz >= 0, get(zb, lax.rem(z + d, nz), h), identity)
                    low_state[h] = apply_map(got, low_state[h], True)
                    if d == ups - 1:
                        near[h] = compose(before_row[h], near[h])
                        own_near[h] = compose(map0[h], near[h])
                else:
                    row_state = apply_map(got, low_state[h], True)
                    fin_send[h] = apply_map(near[h], row_state)
                    sin[h] = apply_map(own_near[h], row_state)
        give.start()
        give.wait_send()
        for group in [y1, y2, y3] + up + dn:
            for a in group:
                a.wait_send()

    h_direct, h_relay = ring(hg, 0, hd_send, hd_recv, hf_send, hf_recv)
    starts = [right3(sin[h]) for h in range(heads)]
    for t in range(chunks):
        rows = slice(t * BLK, (t + 1) * BLK)
        for h in range(heads):
            part = prelim[h, rows, :]
            head_out = dot1(left3(part[:, :BLK]), starts[h]) + part[:, BLK:]
            scaled = head_out * lax.rsqrt(
                jnp.mean(head_out * head_out, axis=-1, keepdims=True) + NORM_FLOOR
            )
            cols = slice(h * BLK, (h + 1) * BLK)
            hg[x, rows, cols] = (scaled * gate[rows, cols]).astype(BF16)
        for way in range(2):
            h_direct(way, t).start()
    for t in range(chunks):
        for way in range(2):
            h_direct(way, t).wait_recv()
            h_relay(way, t).start()
    own_cols.wait()
    @pl.when(c == 1)
    def _():
        for j in range(1, nx):
            handed(j).wait_recv()

    for t in range(chunks):
        rows = slice(t * BLK, (t + 1) * BLK)
        for way in range(2):
            h_relay(way, t).wait_recv()
        rows_all = jnp.concatenate([hg[p, rows, :] for p in range(nx)], axis=1)
        out[rows, :] = dot1(rows_all, col_w[...]).astype(BF16)

    for i in range(nx):
        pre_copy(i).wait_send()
    for t in range(chunks):
        for way in range(2):
            direct(way, t).wait_send()
            relay(way, t).wait_send()
            h_direct(way, t).wait_send()
            h_relay(way, t).wait_send()


def on_device(
    sizes,
    layer_in,
    query_weight,
    key_weight,
    value_weight,
    gate_weight,
    beta_weight,
    decay_weight,
    conv_weight,
    decay_log,
    beta_bias,
    decay_bias,
    norm_gain,
    out_weight,
):
    tokens, feats = layer_in.shape
    depth, width = query_weight.shape
    nz, ny, nx = sizes["z"], sizes["y"], sizes["x"]
    chunks = tokens // BLK
    heads = 2
    hbm = pl.BlockSpec(memory_space=pltpu.HBM)
    vmem = pl.BlockSpec(memory_space=pltpu.VMEM)
    dma = pltpu.SemaphoreType.DMA
    zc = nz - 1
    return pl.pallas_call(
        functools.partial(kernel, sizes),
        out_shape=pltpu.VMEM((tokens, feats), BF16),
        in_specs=[hbm] * 13,
        out_specs=vmem,
        scratch_shapes=[
            pltpu.VMEM((nx, tokens + PRE, feats), BF16),
            pltpu.VMEM((depth, 4 * width + BLK), BF16),
            pltpu.VMEM((nx * width, feats), BF16),
            pltpu.VMEM((heads, BLK, 2 * BLK), F32),
            pltpu.VMEM((heads, 8, 2 * BLK), F32),
            pltpu.VMEM((heads, tokens, 2 * BLK), F32),
            pltpu.VMEM((tokens, width), F32),
            pltpu.VMEM((nx, tokens, width), BF16),
            pltpu.VMEM((heads, BLK + 8, 2 * BLK), F32),
            pltpu.VMEM((heads, BLK + 8, 2 * BLK), F32),
            pltpu.VMEM((ny, heads, BLK + PRE, 2 * BLK), BF16),
            pltpu.VMEM((nz, heads, BLK + PRE, 2 * BLK), BF16),
            pltpu.VMEM((heads, BLK, BLK), F32),
            pltpu.VMEM((heads, BLK, BLK), F32),
            pltpu.VMEM((heads, depth), BF16),
            pltpu.VMEM((heads, depth), BF16),
            pltpu.VMEM((3, 4, width), F32),
            pltpu.VMEM((BLK,), F32),
            pltpu.SMEM((heads,), F32),
            pltpu.SMEM((heads,), F32),
            pltpu.SMEM((heads,), F32),
            dma((13,)),
            dma((nx,)),
            dma((nx,)),
            dma((2, chunks)),
            dma((2, chunks)),
            dma((2, chunks)),
            dma((2, chunks)),
            dma((nx - 1,)),
            dma((nx - 1,)),
            dma((nx - 1,)),
            dma((nx - 1,)),
            dma((2,)),
            dma((2,)),
            dma((3, heads, len(PIECES))),
            dma((3, heads, len(PIECES))),
            dma((zc, heads, len(PIECES))),
            dma((zc, heads, len(PIECES))),
            dma((2, chunks)),
            dma((2, chunks)),
            dma((2, chunks)),
            dma((2, chunks)),
        ],
        compiler_params=pltpu.CompilerParams(
            collective_id=0, has_side_effects=True, vmem_limit_bytes=66519040
        ),
        name="layer",
    )(
        layer_in,
        query_weight,
        key_weight,
        value_weight,
        gate_weight,
        beta_weight.T,
        decay_weight.T,
        conv_weight.transpose(1, 0, 2),
        decay_log,
        beta_bias,
        decay_bias,
        norm_gain,
        out_weight,
    )


def solution(mesh):
    sizes = {"z": 8, "y": 4, "c": 2, "x": mesh.shape["head"]}
    finer = Mesh(
        mesh.devices.reshape(sizes["z"], sizes["y"], sizes["c"], sizes["x"]),
        ("z", "y", "c", "x"),
    )
    return jax.shard_map(
        functools.partial(on_device, sizes),
        mesh=finer,
        in_specs=(
            P(SEQ, "x"),
            P(None, "x"),
            P(None, "x"),
            P(None, "x"),
            P(None, "x"),
            P(None, "x"),
            P(None, "x"),
            P(None, None, "x"),
            P("x"),
            P("x"),
            P("x"),
            P(),
            P("x", None),
        ),
        out_specs=P(SEQ, "x"),
        check_vma=False,
    )
```

```python
import functools

import jax
import jax.numpy as jnp
from jax import lax
from jax.experimental import pallas as pl
from jax.experimental.pallas import tpu as pltpu
from jax.sharding import Mesh
from jax.sharding import PartitionSpec as P

F32 = jnp.float32
BF16 = jnp.bfloat16
MESH = pl.DeviceIdType.MESH
SEQ = ("z", "y", "c")
BLK = 128
HALF = BLK // 2
PRE = 16
SENT = 8
PIECES = ((0, 80), (80, 64))
NORM_FLOOR = 0.0001

NN = (((1,), (0,)), ((), ()))


def dot1(a, b):
    return lax.dot_general(a, b, NN, preferred_element_type=F32)


def halves(a):
    hi = a.astype(BF16)
    lo = (a - hi.astype(F32)).astype(BF16)
    return hi, lo


def left3(a):
    hi, lo = halves(a)
    return jnp.concatenate([hi, hi, lo], axis=1)


def right3(b):
    hi, lo = halves(b)
    return jnp.concatenate([hi, lo, hi], axis=0)


def dot3(a, b):
    return dot1(left3(a), right3(b))


def product(a, b, exact_a=False, exact_b=False):
    if exact_a and exact_b:
        return dot1(a.astype(BF16), b.astype(BF16))
    if exact_a:
        hi, lo = halves(b)
        a = a.astype(BF16)
        return dot1(jnp.concatenate([a, a], axis=1), jnp.concatenate([hi, lo], axis=0))
    if exact_b:
        hi, lo = halves(a)
        b = b.astype(BF16)
        return dot1(jnp.concatenate([hi, lo], axis=1), jnp.concatenate([b, b], axis=0))
    return dot3(a, b)


def sigmoid(v):
    return 1.0 / (1.0 + jnp.exp(-v))


def silu(v):
    return v / (1.0 + jnp.exp(-v))


def softplus(v):
    return jnp.maximum(v, 0.0) + jnp.log(1.0 + jnp.exp(-jnp.abs(v)))


def compose(later, earlier, *exact):
    l2, b2, c2 = later
    l1, b1, c1 = earlier
    moved = product(l2, jnp.concatenate([l1, b1], axis=1), *exact)
    width = l1.shape[1]
    return (
        c2[:, :width] * l1 + c1[:, :width] * l2 - moved[:, :width],
        c2[:, :width] * b1 + b2 - moved[:, width:],
        c1 * c2,
    )


def apply_map(m, state, *exact):
    l, b, c = m
    return c[:, : state.shape[1]] * state - product(l, state, *exact) + b


def pick(flag, m, other):
    return jax.tree.map(lambda a, b: jnp.where(flag, a, b), m, other)


def kernel(
    sizes,
    x_in,
    wq,
    wk,
    wv,
    wg,
    wb_in,
    wd_in,
    conv_in,
    decay_log_in,
    beta_bias_in,
    decay_bias_in,
    norm_gain_in,
    w_out,
    out,
    xg,
    w_all,
    col_w,
    state,
    logsum,
    prelim,
    gate,
    hg,
    sc_send,
    sc_recv,
    yb,
    zb,
    fin_send,
    sin,
    wb,
    wd,
    conv_w,
    norm_gain,
    decay_log,
    beta_bias,
    decay_bias,
    load_sem,
    pre_send,
    pre_recv,
    d_send,
    d_recv,
    f_send,
    f_recv,
    w_send,
    w_recv,
    hand_send,
    hand_recv,
    c_send,
    c_recv,
    y_send,
    y_recv,
    z_send,
    z_recv,
    hd_send,
    hd_recv,
    hf_send,
    hf_recv,
    ready,
):
    nz, ny, nx = sizes["z"], sizes["y"], sizes["x"]
    z = lax.axis_index("z")
    y = lax.axis_index("y")
    c = lax.axis_index("c")
    x = lax.axis_index("x")
    tokens = x_in.shape[0]
    feats = x_in.shape[1]
    chunks = tokens // BLK
    heads = 2
    width = heads * BLK
    right, left = lax.rem(x + 1, nx), lax.rem(x + nx - 1, nx)
    far = lax.rem(x + 2, nx)
    count = nz * ny * 2
    here = (z * ny + y) * 2 + c
    after = lax.rem(here + 1, count)
    prior = lax.rem(here + count - 1, count)

    def place(s, xx):
        return {"z": s // (ny * 2), "y": lax.rem(s // 2, ny), "c": lax.rem(s, 2), "x": xx}

    xg[:, 0:PRE, :] = jnp.zeros((nx, PRE, feats), BF16)

    weights = (wq, wk, wv, wg)
    loads = [pltpu.make_async_copy(x_in, xg.at[x, pl.ds(PRE, tokens), :], load_sem.at[0])]
    loads[0].start()
    for i, w in enumerate(weights):
        cp = pltpu.make_async_copy(
            w, w_all.at[:, pl.ds(i * width, width)], load_sem.at[1 + i]
        )
        cp.start()
        loads.append(cp)
    small_loads = (
        (wb_in, wb),
        (wd_in, wd),
        (conv_in, conv_w),
        (norm_gain_in, norm_gain),
        (decay_log_in, decay_log),
        (beta_bias_in, beta_bias),
        (decay_bias_in, decay_bias),
    )
    for i, (src, dst) in enumerate(small_loads):
        cp = pltpu.make_async_copy(src, dst, load_sem.at[6 + i])
        cp.start()
        loads.append(cp)
    own_cols = pltpu.make_async_copy(
        w_out.at[:, pl.ds(pl.multiple_of(x * feats, feats), feats)],
        col_w.at[pl.ds(pl.multiple_of(x * width, width), width), :],
        load_sem.at[5],
    )
    own_cols.start()

    barrier = pltpu.get_barrier_semaphore()
    up_y, down_y = lax.rem(y + 1, ny), lax.rem(y + ny - 1, ny)
    up_z, down_z = lax.rem(z + 1, nz), lax.rem(z + nz - 1, nz)
    last_z = nz - 1
    has_after = here < count - 1
    has_prior = here > 0

    def enter(who):
        pl.semaphore_signal(barrier, inc=1, device_id=who, device_id_type=MESH)

    always = [{"x": right}, {"x": left}, {"x": far}, {"c": 1 - c}, {"y": up_y}, {"y": down_y}]
    for who in always:
        enter(who)

    @pl.when(has_prior)
    def _():
        for i in range(nx):
            enter(place(prior, i))

    @pl.when(z > 0)
    def _():
        enter({"z": down_z})

    @pl.when(z < last_z)
    def _():
        enter({"z": up_z})

    @pl.when(z == 0)
    def _():
        enter({"z": down_z})

    expected = (
        len(always)
        + nx * has_after.astype(jnp.int32)
        + (z < last_z).astype(jnp.int32)
        + (z > 0).astype(jnp.int32)
        + (z == last_z).astype(jnp.int32)
    )

    state[...] = jnp.zeros_like(state)
    eye = (
        lax.broadcasted_iota(jnp.int32, (BLK, BLK), 0)
        == lax.broadcasted_iota(jnp.int32, (BLK, BLK), 1)
    ).astype(F32)
    for h in range(heads):
        state[h, :, 0:BLK] = eye
    logsum[...] = jnp.zeros_like(logsum)
    pl.semaphore_wait(barrier, expected)

    @pl.when(jnp.logical_and(z == last_z, c == 1))
    def _():
        pl.semaphore_signal(ready, inc=1, device_id={"z": up_z}, device_id_type=MESH)

    loads[0].wait()

    def remote(src, dst, send, recv, who):
        return pltpu.make_async_remote_copy(
            src_ref=src,
            dst_ref=dst,
            send_sem=send,
            recv_sem=recv,
            device_id=who,
            device_id_type=MESH,
        )


    def ring(buf, base, send, recv, relay_send, relay_recv):
        def direct(way, t):
            rows = pl.ds(pl.multiple_of(base + t * BLK, PRE), BLK)
            return remote(
                buf.at[x, rows, :],
                buf.at[x, rows, :],
                send.at[way, t],
                recv.at[way, t],
                {"x": (right, left)[way]},
            )

        def relay(way, t):
            rows = pl.ds(pl.multiple_of(base + t * BLK + way * HALF, PRE), HALF)
            source = (left, right)[way]
            return remote(
                buf.at[source, rows, :],
                buf.at[source, rows, :],
                relay_send.at[way, t],
                relay_recv.at[way, t],
                {"x": (right, left)[way]},
            )

        return direct, relay

    direct, relay = ring(xg, PRE, d_send, d_recv, f_send, f_recv)

    def pre_copy(i):
        return remote(
            xg.at[x, pl.ds(tokens + SENT, SENT), :],
            xg.at[x, pl.ds(SENT, SENT), :],
            pre_send.at[i],
            pre_recv.at[x],
            place(after, i),
        )

    @pl.when(has_after)
    def _():
        for i in range(nx):
            pre_copy(i).start()

    for t in range(2):
        for way in range(2):
            direct(way, t).start()
    for cp in loads[1:]:
        cp.wait()
    depth = wb.shape[1]
    wide_row = lax.broadcasted_iota(jnp.int32, (8, BLK), 0)
    for i in range(depth // BLK):
        cols = slice(i * BLK, (i + 1) * BLK)
        b_rows, d_rows = wb[:, cols].astype(F32), wd[:, cols].astype(F32)
        tile = jnp.where(wide_row == 0, b_rows[0:1], 0.0)
        tile = jnp.where(wide_row == 1, b_rows[1:2], tile)
        tile = jnp.where(wide_row == 2, d_rows[0:1], tile)
        tile = jnp.where(wide_row == 3, d_rows[1:2], tile)
        tile = jnp.concatenate([tile, jnp.zeros((BLK - 8, BLK), F32)], axis=0)
        w_all[cols, 4 * width :] = jnp.transpose(tile).astype(BF16)

    row_i = lax.broadcasted_iota(jnp.int32, (BLK, BLK), 0)
    col_i = lax.broadcasted_iota(jnp.int32, (BLK, BLK), 1)
    differ = jnp.bitwise_xor(row_i, col_i)
    within = row_i >= col_i
    before = row_i > col_i

    lane = lax.broadcasted_iota(jnp.int32, (1, BLK), 1)
    bias_row = jnp.where(lane == 0, beta_bias[0], 0.0)
    bias_row = jnp.where(lane == 1, beta_bias[1], bias_row)
    bias_row = jnp.where(lane == 2, decay_bias[0], bias_row)
    bias_row = jnp.where(lane == 3, decay_bias[1], bias_row)
    rate_row = jnp.where(lane == 2, decay_log[0], -200.0)
    rate_row = jnp.exp(jnp.where(lane == 3, decay_log[1], rate_row))
    gain_row = norm_gain[...].reshape(1, BLK)

    def unit_rows(v):
        return v * lax.rsqrt(jnp.sum(v * v, axis=-1, keepdims=True) + 1.0)

    def chunk(t):
        start = pl.multiple_of(t * BLK, BLK)
        rows = pl.ds(start, BLK + PRE)
        xs = jnp.concatenate([xg[p, rows, :] for p in range(nx)], axis=1)
        first = jnp.logical_and(here == 0, t == 0)
        ext_row = lax.broadcasted_iota(jnp.int32, (BLK + PRE, 3 * width), 0)
        raw = dot1(xs, w_all[...])
        qkv = raw[:, 0 : 3 * width]
        qkv = jnp.where(jnp.logical_and(first, ext_row < PRE), 0.0, qkv)
        taps = [
            jnp.concatenate([conv_w[i, s : s + 1, :] for i in range(3)], axis=1)
            for s in range(4)
        ]
        mixed = taps[0] * qkv
        for s in range(1, 4):
            mixed = mixed + taps[s] * pltpu.roll(qkv, s, 0)
        mixed = silu(mixed[PRE:])
        out_rows = pl.ds(start, BLK)
        gates = silu(raw[PRE:, 3 * width : 4 * width])
        for h in range(heads):
            gate[out_rows, h * BLK : (h + 1) * BLK] = (
                gates[:, h * BLK : (h + 1) * BLK] * gain_row
            )
        small = raw[PRE:, 4 * width :] + bias_row
        betas = sigmoid(small)
        steps = -rate_row * softplus(small)
        s_hi = steps.astype(BF16)
        rest = steps - s_hi.astype(F32)
        s_mid = rest.astype(BF16)
        s_lo = (rest - s_mid.astype(F32)).astype(BF16)
        tri = within.astype(F32).astype(BF16)
        total = dot1(
            jnp.concatenate([tri, tri, tri], axis=1),
            jnp.concatenate([s_hi, s_mid, s_lo], axis=0),
        )
        total_t = jnp.transpose(total)
        both = []
        for h in range(heads):
            cols = slice(h * BLK, (h + 1) * BLK)
            q = unit_rows(mixed[:, h * BLK : (h + 1) * BLK])
            k = unit_rows(mixed[:, width + h * BLK : width + (h + 1) * BLK])
            v = mixed[:, 2 * width + h * BLK : 2 * width + (h + 1) * BLK]
            beta = betas[:, h : h + 1]
            run_c = total[:, 2 + h : 3 + h]
            run_r = total_t[2 + h : 3 + h, :]
            end = run_r[:, BLK - 1 : BLK]
            decay = jnp.where(within, jnp.exp(jnp.minimum(run_c - run_r, 0.0)), 0.0)
            kt = jnp.transpose(k)
            scores = dot3(jnp.concatenate([k, q], axis=0), kt)
            low = jnp.where(before, beta * decay * scores[:BLK], 0.0)
            mix = decay * scores[BLK:]
            grow = jnp.exp(run_c)
            ext = state[h]
            read = dot3(
                jnp.concatenate([(beta * grow) * k, grow * q], axis=0), ext
            )
            right_side = (
                jnp.concatenate([jnp.zeros_like(v), beta * v], axis=1) - read[:BLK]
            )
            both.append((low, mix, right_side, read[BLK:], kt, run_r, end, ext))
        first_links = [jnp.where(differ == 1, b[0], 0.0) for b in both]
        inv = [jnp.where(row_i == col_i, 1.0, 0.0) - m for m in first_links]
        rest = []
        for b, m in zip(both, first_links):
            later = jnp.where(differ > 1, b[0], 0.0)
            rest.append(later - dot3(later, m))
        w = 2
        while w < BLK:
            linking = jnp.logical_and(differ >= w, differ < 2 * w)
            links = [right3(jnp.where(linking, r, 0.0)) for r in rest]
            if 2 * w < BLK:
                later = [jnp.where(differ >= 2 * w, r, 0.0) for r in rest]
                stacked = [
                    jnp.concatenate([r, a], axis=0) for r, a in zip(later, inv)
                ]
                moved = [s - dot1(left3(s), m) for s, m in zip(stacked, links)]
                rest = [m[:BLK] for m in moved]
                inv = [m[BLK:] for m in moved]
            else:
                inv = [a - dot1(left3(a), m) for a, m in zip(inv, links)]
            w *= 2
        for h in range(heads):
            low, mix, right_side, carried, kt, run_r, end, ext = both[h]
            solved = dot3(inv[h], right_side)
            solved3 = right3(solved)
            prelim[h, out_rows, :] = carried + dot1(left3(mix), solved3)
            weighted = kt * jnp.exp(end - run_r)
            state[h] = jnp.exp(end) * ext + dot1(left3(weighted), solved3)
            logsum[h] = logsum[h] + jnp.broadcast_to(end, logsum.shape[1:])

    def step(t, carry):
        @pl.when(t < chunks)
        def _():
            direct(0, t).wait_recv()
            direct(1, t).wait_recv()
            relay(0, t).start()
            relay(1, t).start()

        @pl.when(t < chunks - 2)
        def _():
            direct(0, t + 2).start()
            direct(1, t + 2).start()

        @pl.when(jnp.logical_and(t == 0, has_prior))
        def _():
            for i in range(nx):
                remote(
                    xg.at[i, pl.ds(tokens + SENT, SENT), :],
                    xg.at[i, pl.ds(SENT, SENT), :],
                    pre_send.at[i],
                    pre_recv.at[i],
                    place(after, i),
                ).wait_recv()

        @pl.when(t > 0)
        def _():
            relay(0, t - 1).wait_recv()
            relay(1, t - 1).wait_recv()
            chunk(t - 1)

        return carry

    lax.fori_loop(0, chunks + 1, step, 0)

    def columns(j):
        who = lax.rem(x + j, nx)
        return remote(
            w_out.at[:, pl.ds(pl.multiple_of(who * feats, feats), feats)],
            col_w.at[pl.ds(pl.multiple_of(x * width, width), width), :],
            w_send.at[j - 1],
            w_recv.at[j - 1],
            {"x": who},
        )

    def handed(j):
        rows = pl.ds(pl.multiple_of(lax.rem(x + nx - j, nx) * width, width), width)
        return remote(
            col_w.at[rows, :],
            col_w.at[rows, :],
            hand_send.at[j - 1],
            hand_recv.at[j - 1],
            {"c": 1 - c},
        )

    @pl.when(c == 0)
    def _():
        for j in range(1, nx):
            columns(j).start()


    def own_map(h):
        ext = state[h]
        keep = jnp.exp(logsum[h, 0:1, :])
        return (keep[:, :BLK] * eye - ext[:, :BLK], ext[:, BLK:], keep)

    swap = remote(sc_send, sc_recv, c_send.at[0], c_recv.at[0], {"c": 1 - c})
    give = remote(fin_send, sin, c_send.at[1], c_recv.at[1], {"c": 1 - c})

    @pl.when(c == 0)
    def _():
        for h in range(heads):
            l, b, keep = own_map(h)
            sc_send[h, 0:BLK, 0:BLK] = l
            sc_send[h, 0:BLK, BLK:] = b
            sc_send[h, BLK:, :] = jnp.broadcast_to(keep, (8, 2 * BLK))
        swap.start()
        swap.wait_send()
        for j in range(1, nx):
            columns(j).wait_recv()
            handed(j).start()
        for j in range(1, nx):
            columns(j).wait_send()
            handed(j).wait_send()
        give.wait_recv()

    zero = jnp.zeros((BLK, BLK), F32)
    one_row = jnp.ones((1, 2 * BLK), F32)
    identity = (zero, zero, one_row)
    each = range(heads)

    def put(buf, slot, m, h):
        l, b, keep = m
        buf[slot, h, 0:BLK, 0:BLK] = l.astype(BF16)
        buf[slot, h, 0:BLK, BLK:] = b.astype(BF16)
        hi, lo = halves(keep)
        tail = lax.broadcasted_iota(jnp.int32, (PRE, 2 * BLK), 0)
        buf[slot, h, BLK:, :] = jnp.where(
            tail == 0,
            jnp.broadcast_to(hi.astype(F32), (PRE, 2 * BLK)),
            jnp.broadcast_to(lo.astype(F32), (PRE, 2 * BLK)),
        ).astype(BF16)

    def get(buf, slot, h):
        tail = buf[slot, h, BLK:, :].astype(F32)
        return (
            buf[slot, h, 0:BLK, 0:BLK].astype(F32),
            buf[slot, h, 0:BLK, BLK:].astype(F32),
            tail[0:1] + tail[1:2],
        )

    def pieces(buf, slot, send, recv, j, who):
        made = []
        for h in each:
            for p, (at, rows) in enumerate(PIECES):
                made.append(
                    remote(
                        buf.at[slot, h, pl.ds(at, rows), :],
                        buf.at[slot, h, pl.ds(at, rows), :],
                        send.at[j, h, p],
                        recv.at[j, h, p],
                        who,
                    )
                )
        return made

    @pl.when(c == 1)
    def _():
        own = [own_map(h) for h in each]
        swap.wait_recv()
        map0 = [
            (sc_recv[h, 0:BLK, 0:BLK], sc_recv[h, 0:BLK, BLK:], sc_recv[h, BLK : BLK + 1, :])
            for h in each
        ]
        for h in each:
            put(yb, y, compose(own[h], map0[h]), h)

        y1 = pieces(yb, y, y_send, y_recv, 0, {"y": up_y})
        y2 = pieces(yb, y, y_send, y_recv, 1, {"y": down_y})
        y3 = pieces(yb, down_y, y_send, y_recv, 2, {"y": up_y})
        for a, b in zip(y1, y2):
            a.start()
            b.start()
        for a, b in zip(y1, y3):
            a.wait_recv()
            b.start()
        for b in y2:
            b.wait_recv()
        for b in y3:
            b.wait_recv()
        before_row = []
        for h in each:
            maps = [get(yb, j, h) for j in range(ny)]
            low_pair = compose(maps[1], maps[0], True, True)
            high_pair = compose(maps[3], maps[2], True, True)
            triple = compose(maps[2], low_pair, True)
            run = compose(high_pair, low_pair)
            prefix = pick(y == 0, identity, maps[0])
            prefix = pick(y == 2, low_pair, prefix)
            prefix = pick(y == 3, triple, prefix)
            before_row.append(prefix)
            put(zb, z, run, h)

        ups, downs = nz // 2, nz - 1 - nz // 2
        up = [
            pieces(zb, lax.rem(z + nz - j, nz), z_send, z_recv, j, {"z": up_z})
            for j in range(ups)
        ]
        dn = [
            pieces(zb, lax.rem(z + j, nz), z_send, z_recv, ups + j, {"z": down_z})
            for j in range(downs)
        ]
        near = [identity] * heads
        low_state = [zero] * heads
        own_near = [identity] * heads
        def guarded(flag, copies, wait=False):
            @pl.when(flag)
            def _():
                for a in copies:
                    if wait:
                        a.wait_send()
                    else:
                        a.start()

        sends_up = [jnp.logical_and(z < last_z, z >= j) for j in range(ups)]
        sends_dn = [lax.rem(z + j, nz) < downs for j in range(downs)]
        guarded(sends_up[0], up[0])

        @pl.when(z == 0)
        def _():
            pl.semaphore_wait(ready, 1)

        guarded(sends_dn[0], dn[0])
        for j in range(ups):
            for p in range(len(up[0])):

                @pl.when(z > j)
                def _():
                    up[j][p].wait_recv()

                if j + 1 < ups:
                    guarded(sends_up[j + 1], [up[j + 1][p]])
                if j < downs:

                    @pl.when(lax.rem(z + 1 + j, nz) < downs)
                    def _():
                        dn[j][p].wait_recv()
                        if j + 1 < downs:
                            dn[j + 1][p].start()

            d = j + 1
            for h in each:
                got = pick(z - d >= 0, get(zb, lax.rem(z + nz - d, nz), h), identity)
                if d < ups:
                    near[h] = compose(near[h], got, False, True)
                    got = pick(z + d - nz >= 0, get(zb, lax.rem(z + d, nz), h), identity)
                    low_state[h] = apply_map(got, low_state[h], True)
                    if d == ups - 1:
                        near[h] = compose(before_row[h], near[h])
                        own_near[h] = compose(map0[h], near[h])
                else:
                    row_state = apply_map(got, low_state[h], True)
                    fin_send[h] = apply_map(near[h], row_state)
                    sin[h] = apply_map(own_near[h], row_state)
        give.start()
        give.wait_send()
        for group in [y1, y2, y3]:
            for a in group:
                a.wait_send()
        for j in range(ups):
            guarded(sends_up[j], up[j], True)
        for j in range(downs):
            guarded(sends_dn[j], dn[j], True)

    h_direct, h_relay = ring(hg, 0, hd_send, hd_recv, hf_send, hf_recv)
    starts = [right3(sin[h]) for h in range(heads)]
    for t in range(chunks):
        rows = slice(t * BLK, (t + 1) * BLK)
        for h in range(heads):
            part = prelim[h, rows, :]
            head_out = dot1(left3(part[:, :BLK]), starts[h]) + part[:, BLK:]
            scaled = head_out * lax.rsqrt(
                jnp.mean(head_out * head_out, axis=-1, keepdims=True) + NORM_FLOOR
            )
            cols = slice(h * BLK, (h + 1) * BLK)
            hg[x, rows, cols] = (scaled * gate[rows, cols]).astype(BF16)
        for way in range(2):
            h_direct(way, t).start()
    for t in range(chunks):
        for way in range(2):
            h_direct(way, t).wait_recv()
            h_relay(way, t).start()
    own_cols.wait()
    @pl.when(c == 1)
    def _():
        for j in range(1, nx):
            handed(j).wait_recv()

    for t in range(chunks):
        rows = slice(t * BLK, (t + 1) * BLK)
        for way in range(2):
            h_relay(way, t).wait_recv()
        rows_all = jnp.concatenate([hg[p, rows, :] for p in range(nx)], axis=1)
        out[rows, :] = dot1(rows_all, col_w[...]).astype(BF16)

    @pl.when(has_after)
    def _():
        for i in range(nx):
            pre_copy(i).wait_send()

    for t in range(chunks):
        for way in range(2):
            direct(way, t).wait_send()
            relay(way, t).wait_send()
            h_direct(way, t).wait_send()
            h_relay(way, t).wait_send()


def on_device(
    sizes,
    layer_in,
    query_weight,
    key_weight,
    value_weight,
    gate_weight,
    beta_weight,
    decay_weight,
    conv_weight,
    decay_log,
    beta_bias,
    decay_bias,
    norm_gain,
    out_weight,
):
    tokens, feats = layer_in.shape
    depth, width = query_weight.shape
    nz, ny, nx = sizes["z"], sizes["y"], sizes["x"]
    chunks = tokens // BLK
    heads = 2
    hbm = pl.BlockSpec(memory_space=pltpu.HBM)
    vmem = pl.BlockSpec(memory_space=pltpu.VMEM)
    dma = pltpu.SemaphoreType.DMA
    zc = nz - 1
    return pl.pallas_call(
        functools.partial(kernel, sizes),
        out_shape=pltpu.VMEM((tokens, feats), BF16),
        in_specs=[hbm] * 13,
        out_specs=vmem,
        scratch_shapes=[
            pltpu.VMEM((nx, tokens + PRE, feats), BF16),
            pltpu.VMEM((depth, 4 * width + BLK), BF16),
            pltpu.VMEM((nx * width, feats), BF16),
            pltpu.VMEM((heads, BLK, 2 * BLK), F32),
            pltpu.VMEM((heads, 8, 2 * BLK), F32),
            pltpu.VMEM((heads, tokens, 2 * BLK), F32),
            pltpu.VMEM((tokens, width), F32),
            pltpu.VMEM((nx, tokens, width), BF16),
            pltpu.VMEM((heads, BLK + 8, 2 * BLK), F32),
            pltpu.VMEM((heads, BLK + 8, 2 * BLK), F32),
            pltpu.VMEM((ny, heads, BLK + PRE, 2 * BLK), BF16),
            pltpu.VMEM((nz, heads, BLK + PRE, 2 * BLK), BF16),
            pltpu.VMEM((heads, BLK, BLK), F32),
            pltpu.VMEM((heads, BLK, BLK), F32),
            pltpu.VMEM((heads, depth), BF16),
            pltpu.VMEM((heads, depth), BF16),
            pltpu.VMEM((3, 4, width), F32),
            pltpu.VMEM((BLK,), F32),
            pltpu.SMEM((heads,), F32),
            pltpu.SMEM((heads,), F32),
            pltpu.SMEM((heads,), F32),
            dma((13,)),
            dma((nx,)),
            dma((nx,)),
            dma((2, chunks)),
            dma((2, chunks)),
            dma((2, chunks)),
            dma((2, chunks)),
            dma((nx - 1,)),
            dma((nx - 1,)),
            dma((nx - 1,)),
            dma((nx - 1,)),
            dma((2,)),
            dma((2,)),
            dma((3, heads, len(PIECES))),
            dma((3, heads, len(PIECES))),
            dma((zc, heads, len(PIECES))),
            dma((zc, heads, len(PIECES))),
            dma((2, chunks)),
            dma((2, chunks)),
            dma((2, chunks)),
            dma((2, chunks)),
            pltpu.SemaphoreType.REGULAR,
        ],
        compiler_params=pltpu.CompilerParams(
            collective_id=0, has_side_effects=True, vmem_limit_bytes=66519040
        ),
        name="layer",
    )(
        layer_in,
        query_weight,
        key_weight,
        value_weight,
        gate_weight,
        beta_weight.T,
        decay_weight.T,
        conv_weight.transpose(1, 0, 2),
        decay_log,
        beta_bias,
        decay_bias,
        norm_gain,
        out_weight,
    )


def solution(mesh):
    sizes = {"z": 8, "y": 4, "c": 2, "x": mesh.shape["head"]}
    finer = Mesh(
        mesh.devices.reshape(sizes["z"], sizes["y"], sizes["c"], sizes["x"]),
        ("z", "y", "c", "x"),
    )
    return jax.shard_map(
        functools.partial(on_device, sizes),
        mesh=finer,
        in_specs=(
            P(SEQ, "x"),
            P(None, "x"),
            P(None, "x"),
            P(None, "x"),
            P(None, "x"),
            P(None, "x"),
            P(None, "x"),
            P(None, None, "x"),
            P("x"),
            P("x"),
            P("x"),
            P(),
            P("x", None),
        ),
        out_specs=P(SEQ, "x"),
        check_vma=False,
    )
```

```python
import functools

import jax
import jax.numpy as jnp
from jax import lax
from jax.experimental import pallas as pl
from jax.experimental.pallas import tpu as pltpu
from jax.sharding import Mesh
from jax.sharding import PartitionSpec as P

F32 = jnp.float32
BF16 = jnp.bfloat16
MESH = pl.DeviceIdType.MESH
SEQ = ("z", "y", "c")
BLK = 128
HALF = BLK // 2
PRE = 16
SENT = 8
PIECES = ((0, 48), (48, 48), (96, 48))
NORM_FLOOR = 0.0001

NN = (((1,), (0,)), ((), ()))


def dot1(a, b):
    return lax.dot_general(a, b, NN, preferred_element_type=F32)


def halves(a):
    hi = a.astype(BF16)
    lo = (a - hi.astype(F32)).astype(BF16)
    return hi, lo


def left3(a):
    hi, lo = halves(a)
    return jnp.concatenate([hi, hi, lo], axis=1)


def right3(b):
    hi, lo = halves(b)
    return jnp.concatenate([hi, lo, hi], axis=0)


def dot3(a, b):
    return dot1(left3(a), right3(b))


def product(a, b, exact_a=False, exact_b=False):
    if exact_a and exact_b:
        return dot1(a.astype(BF16), b.astype(BF16))
    if exact_a:
        hi, lo = halves(b)
        a = a.astype(BF16)
        return dot1(jnp.concatenate([a, a], axis=1), jnp.concatenate([hi, lo], axis=0))
    if exact_b:
        hi, lo = halves(a)
        b = b.astype(BF16)
        return dot1(jnp.concatenate([hi, lo], axis=1), jnp.concatenate([b, b], axis=0))
    return dot3(a, b)


def sigmoid(v):
    return 1.0 / (1.0 + jnp.exp(-v))


def silu(v):
    return v / (1.0 + jnp.exp(-v))


def softplus(v):
    return jnp.maximum(v, 0.0) + jnp.log(1.0 + jnp.exp(-jnp.abs(v)))


def compose(later, earlier, *exact):
    l2, b2, c2 = later
    l1, b1, c1 = earlier
    moved = product(l2, jnp.concatenate([l1, b1], axis=1), *exact)
    width = l1.shape[1]
    return (
        c2[:, :width] * l1 + c1[:, :width] * l2 - moved[:, :width],
        c2[:, :width] * b1 + b2 - moved[:, width:],
        c1 * c2,
    )


def apply_map(m, state, *exact):
    l, b, c = m
    return c[:, : state.shape[1]] * state - product(l, state, *exact) + b


def pick(flag, m, other):
    return jax.tree.map(lambda a, b: jnp.where(flag, a, b), m, other)


def kernel(
    sizes,
    x_in,
    wq,
    wk,
    wv,
    wg,
    wb_in,
    wd_in,
    conv_in,
    decay_log_in,
    beta_bias_in,
    decay_bias_in,
    norm_gain_in,
    w_out,
    out,
    xg,
    w_all,
    col_w,
    state,
    logsum,
    prelim,
    gate,
    hg,
    sc_send,
    sc_recv,
    yb,
    zb,
    fin_send,
    sin,
    wb,
    wd,
    conv_w,
    norm_gain,
    decay_log,
    beta_bias,
    decay_bias,
    kept_q,
    kept_g,
    kept_total,
    kept_kt,
    kept_state,
    kept_u,
    load_sem,
    pre_send,
    pre_recv,
    d_send,
    d_recv,
    f_send,
    f_recv,
    w_send,
    w_recv,
    hand_send,
    hand_recv,
    c_send,
    c_recv,
    y_send,
    y_recv,
    z_send,
    z_recv,
    hd_send,
    hd_recv,
    hf_send,
    hf_recv,
    ready,
):
    nz, ny, nx = sizes["z"], sizes["y"], sizes["x"]
    z = lax.axis_index("z")
    y = lax.axis_index("y")
    c = lax.axis_index("c")
    x = lax.axis_index("x")
    tokens = x_in.shape[0]
    feats = x_in.shape[1]
    chunks = tokens // BLK
    heads = 2
    width = heads * BLK
    right, left = lax.rem(x + 1, nx), lax.rem(x + nx - 1, nx)
    far = lax.rem(x + 2, nx)
    count = nz * ny * 2
    here = (z * ny + y) * 2 + c
    after = lax.rem(here + 1, count)
    prior = lax.rem(here + count - 1, count)

    def place(s, xx):
        return {"z": s // (ny * 2), "y": lax.rem(s // 2, ny), "c": lax.rem(s, 2), "x": xx}

    xg[:, 0:PRE, :] = jnp.zeros((nx, PRE, feats), BF16)

    weights = (wq, wk, wv, wg)
    loads = [pltpu.make_async_copy(x_in, xg.at[x, pl.ds(PRE, tokens), :], load_sem.at[0])]
    loads[0].start()
    for i, w in enumerate(weights):
        cp = pltpu.make_async_copy(
            w, w_all.at[:, pl.ds(i * width, width)], load_sem.at[1 + i]
        )
        cp.start()
        loads.append(cp)
    small_loads = (
        (wb_in, wb),
        (wd_in, wd),
        (conv_in, conv_w),
        (norm_gain_in, norm_gain),
        (decay_log_in, decay_log),
        (beta_bias_in, beta_bias),
        (decay_bias_in, decay_bias),
    )
    for i, (src, dst) in enumerate(small_loads):
        cp = pltpu.make_async_copy(src, dst, load_sem.at[6 + i])
        cp.start()
        loads.append(cp)
    own_cols = pltpu.make_async_copy(
        w_out.at[:, pl.ds(pl.multiple_of(x * feats, feats), feats)],
        col_w.at[pl.ds(pl.multiple_of(x * width, width), width), :],
        load_sem.at[5],
    )
    own_cols.start()

    barrier = pltpu.get_barrier_semaphore()
    up_y, down_y = lax.rem(y + 1, ny), lax.rem(y + ny - 1, ny)
    up_z, down_z = lax.rem(z + 1, nz), lax.rem(z + nz - 1, nz)
    last_z = nz - 1
    has_after = here < count - 1
    has_prior = here > 0

    def enter(who):
        pl.semaphore_signal(barrier, inc=1, device_id=who, device_id_type=MESH)

    always = [{"x": right}, {"x": left}, {"x": far}, {"c": 1 - c}, {"y": up_y}, {"y": down_y}]
    for who in always:
        enter(who)

    @pl.when(has_prior)
    def _():
        for i in range(nx):
            enter(place(prior, i))

    @pl.when(z > 0)
    def _():
        enter({"z": down_z})

    @pl.when(z < last_z)
    def _():
        enter({"z": up_z})

    @pl.when(z == 0)
    def _():
        enter({"z": down_z})

    expected = (
        len(always)
        + nx * has_after.astype(jnp.int32)
        + (z < last_z).astype(jnp.int32)
        + (z > 0).astype(jnp.int32)
        + (z == last_z).astype(jnp.int32)
    )

    state[...] = jnp.zeros_like(state)
    eye = (
        lax.broadcasted_iota(jnp.int32, (BLK, BLK), 0)
        == lax.broadcasted_iota(jnp.int32, (BLK, BLK), 1)
    ).astype(F32)
    for h in range(heads):
        state[h, :, 0:BLK] = eye
    logsum[...] = jnp.zeros_like(logsum)
    pl.semaphore_wait(barrier, expected)

    @pl.when(jnp.logical_and(z == last_z, c == 1))
    def _():
        pl.semaphore_signal(ready, inc=1, device_id={"z": up_z}, device_id_type=MESH)

    loads[0].wait()

    def remote(src, dst, send, recv, who):
        return pltpu.make_async_remote_copy(
            src_ref=src,
            dst_ref=dst,
            send_sem=send,
            recv_sem=recv,
            device_id=who,
            device_id_type=MESH,
        )


    def ring(buf, base, send, recv, relay_send, relay_recv):
        def direct(way, t):
            rows = pl.ds(pl.multiple_of(base + t * BLK, PRE), BLK)
            return remote(
                buf.at[x, rows, :],
                buf.at[x, rows, :],
                send.at[way, t],
                recv.at[way, t],
                {"x": (right, left)[way]},
            )

        def relay(way, t):
            rows = pl.ds(pl.multiple_of(base + t * BLK + way * HALF, PRE), HALF)
            source = (left, right)[way]
            return remote(
                buf.at[source, rows, :],
                buf.at[source, rows, :],
                relay_send.at[way, t],
                relay_recv.at[way, t],
                {"x": (right, left)[way]},
            )

        return direct, relay

    direct, relay = ring(xg, PRE, d_send, d_recv, f_send, f_recv)
    final = chunks - 1

    def last(way, p):
        half = way if p == 0 else 1 - way
        rows = pl.ds(PRE + final * BLK + half * HALF, HALF)
        return remote(
            xg.at[x, rows, :],
            xg.at[x, rows, :],
            d_send.at[way, final + p],
            d_recv.at[way, final + p],
            {"x": (right, left)[way]},
        )

    def pre_copy(i):
        return remote(
            xg.at[x, pl.ds(tokens + SENT, SENT), :],
            xg.at[x, pl.ds(SENT, SENT), :],
            pre_send.at[i],
            pre_recv.at[x],
            place(after, i),
        )

    @pl.when(has_after)
    def _():
        for i in range(nx):
            pre_copy(i).start()

    for t in range(2):
        for way in range(2):
            direct(way, t).start()
    for cp in loads[1:]:
        cp.wait()
    depth = wb.shape[1]
    wide_row = lax.broadcasted_iota(jnp.int32, (8, BLK), 0)
    for i in range(depth // BLK):
        cols = slice(i * BLK, (i + 1) * BLK)
        b_rows, d_rows = wb[:, cols].astype(F32), wd[:, cols].astype(F32)
        tile = jnp.where(wide_row == 0, b_rows[0:1], 0.0)
        tile = jnp.where(wide_row == 1, b_rows[1:2], tile)
        tile = jnp.where(wide_row == 2, d_rows[0:1], tile)
        tile = jnp.where(wide_row == 3, d_rows[1:2], tile)
        tile = jnp.concatenate([tile, jnp.zeros((BLK - 8, BLK), F32)], axis=0)
        w_all[cols, 4 * width :] = jnp.transpose(tile).astype(BF16)

    row_i = lax.broadcasted_iota(jnp.int32, (BLK, BLK), 0)
    col_i = lax.broadcasted_iota(jnp.int32, (BLK, BLK), 1)
    differ = jnp.bitwise_xor(row_i, col_i)
    within = row_i >= col_i
    before = row_i > col_i

    lane = lax.broadcasted_iota(jnp.int32, (1, BLK), 1)
    bias_row = jnp.where(lane == 0, beta_bias[0], 0.0)
    bias_row = jnp.where(lane == 1, beta_bias[1], bias_row)
    bias_row = jnp.where(lane == 2, decay_bias[0], bias_row)
    bias_row = jnp.where(lane == 3, decay_bias[1], bias_row)
    rate_row = jnp.where(lane == 2, decay_log[0], -200.0)
    rate_row = jnp.exp(jnp.where(lane == 3, decay_log[1], rate_row))
    gain_row = norm_gain[...].reshape(1, BLK)

    def unit_rows(v):
        return v * lax.rsqrt(jnp.sum(v * v, axis=-1, keepdims=True) + 1.0)

    def mix_taps(which, values):
        taps = [
            jnp.concatenate([conv_w[i, s : s + 1, :] for i in which], axis=1)
            for s in range(4)
        ]
        mixed = taps[0] * values
        for s in range(1, 4):
            mixed = mixed + taps[s] * pltpu.roll(values, s, 0)
        return silu(mixed[PRE:])

    def chunk(t):
        start = pl.multiple_of(t * BLK, BLK)
        rows = pl.ds(start, BLK + PRE)
        xs = jnp.concatenate([xg[p, rows, :] for p in range(nx)], axis=1)
        first = jnp.logical_and(here == 0, t == 0)
        ext_row = lax.broadcasted_iota(jnp.int32, (BLK + PRE, 3 * width), 0)
        raw = dot1(xs, w_all[...])
        qkv = raw[:, 0 : 3 * width]
        qkv = jnp.where(jnp.logical_and(first, ext_row < PRE), 0.0, qkv)
        kept_q[t] = qkv[:, 0:width]
        kept_g[t] = raw[PRE:, 3 * width : 4 * width]
        mixed = mix_taps((1, 2), qkv[:, width:])
        small = raw[PRE:, 4 * width :] + bias_row
        betas = sigmoid(small)
        steps = -rate_row * softplus(small)
        s_hi = steps.astype(BF16)
        rest = steps - s_hi.astype(F32)
        s_mid = rest.astype(BF16)
        s_lo = (rest - s_mid.astype(F32)).astype(BF16)
        tri = within.astype(F32).astype(BF16)
        total = dot1(
            jnp.concatenate([tri, tri, tri], axis=1),
            jnp.concatenate([s_hi, s_mid, s_lo], axis=0),
        )
        total_t = jnp.transpose(total)
        kept_total[t, 0] = total
        kept_total[t, 1] = total_t
        both = []
        for h in range(heads):
            k = unit_rows(mixed[:, h * BLK : (h + 1) * BLK])
            v = mixed[:, width + h * BLK : width + (h + 1) * BLK]
            beta = betas[:, h : h + 1]
            run_c = total[:, 2 + h : 3 + h]
            run_r = total_t[2 + h : 3 + h, :]
            end = run_r[:, BLK - 1 : BLK]
            decay = jnp.where(within, jnp.exp(jnp.minimum(run_c - run_r, 0.0)), 0.0)
            kt = jnp.transpose(k)
            low = jnp.where(before, beta * decay * dot3(k, kt), 0.0)
            ext = state[h]
            read = dot3((beta * jnp.exp(run_c)) * k, ext)
            right_side = jnp.concatenate([jnp.zeros_like(v), beta * v], axis=1) - read
            kept_kt[t, h] = kt
            kept_state[t, h] = ext
            both.append((low, right_side, kt, run_r, end, ext))
        first_links = [jnp.where(differ == 1, b[0], 0.0) for b in both]
        inv = [jnp.where(row_i == col_i, 1.0, 0.0) - m for m in first_links]
        rest = []
        for b, m in zip(both, first_links):
            later = jnp.where(differ > 1, b[0], 0.0)
            rest.append(later - product(later, m, False, True))
        w = 2
        while w < BLK:
            linking = jnp.logical_and(differ >= w, differ < 2 * w)
            links = [jnp.where(linking, r, 0.0) for r in rest]
            if 2 * w < BLK:
                later = [jnp.where(differ >= 2 * w, r, 0.0) for r in rest]
                stacked = [
                    jnp.concatenate([r, a], axis=0) for r, a in zip(later, inv)
                ]
                moved = [
                    s - product(s, m, False, True) for s, m in zip(stacked, links)
                ]
                rest = [m[:BLK] for m in moved]
                inv = [m[BLK:] for m in moved]
            else:
                inv = [a - product(a, m, False, True) for a, m in zip(inv, links)]
            w *= 2
        for h in range(heads):
            low, right_side, kt, run_r, end, ext = both[h]
            solved = dot3(inv[h], right_side)
            kept_u[t, h] = solved
            weighted = kt * jnp.exp(end - run_r)
            state[h] = jnp.exp(end) * ext + dot3(weighted, solved)
            logsum[h] = logsum[h] + jnp.broadcast_to(end, logsum.shape[1:])

    def reading(t):
        start = t * BLK if isinstance(t, int) else pl.multiple_of(t * BLK, BLK)
        out_rows = pl.ds(start, BLK)
        gates = silu(kept_g[t])
        mixed = mix_taps((0,), kept_q[t])
        total, total_t = kept_total[t, 0], kept_total[t, 1]
        for h in range(heads):
            cols = slice(h * BLK, (h + 1) * BLK)
            gate[out_rows, cols] = gates[:, cols] * gain_row
            q = unit_rows(mixed[:, cols])
            run_c = total[:, 2 + h : 3 + h]
            run_r = total_t[2 + h : 3 + h, :]
            decay = jnp.where(within, jnp.exp(jnp.minimum(run_c - run_r, 0.0)), 0.0)
            mix = decay * dot3(q, kept_kt[t, h])
            prelim[h, out_rows, :] = dot3(jnp.exp(run_c) * q, kept_state[t, h]) + dot3(
                mix, kept_u[t, h]
            )

    def step(t, carry):
        @pl.when(t < final)
        def _():
            direct(0, t).wait_recv()
            direct(1, t).wait_recv()

        @pl.when(t == final)
        def _():
            last(0, 0).wait_recv()
            last(1, 0).wait_recv()

        @pl.when(t < chunks)
        def _():
            relay(0, t).start()
            relay(1, t).start()

        @pl.when(t < final - 2)
        def _():
            direct(0, t + 2).start()
            direct(1, t + 2).start()

        @pl.when(t == final - 2)
        def _():
            last(0, 0).start()
            last(1, 0).start()

        @pl.when(t == final - 1)
        def _():
            last(0, 1).start()
            last(1, 1).start()

        @pl.when(t == chunks)
        def _():
            last(0, 1).wait_recv()
            last(1, 1).wait_recv()

        @pl.when(jnp.logical_and(t == 0, has_prior))
        def _():
            for i in range(nx):
                remote(
                    xg.at[i, pl.ds(tokens + SENT, SENT), :],
                    xg.at[i, pl.ds(SENT, SENT), :],
                    pre_send.at[i],
                    pre_recv.at[i],
                    place(after, i),
                ).wait_recv()

        @pl.when(jnp.logical_and(t > 1, t < chunks))
        def _():
            reading(t - 2)

        @pl.when(t > 0)
        def _():
            relay(0, t - 1).wait_recv()
            relay(1, t - 1).wait_recv()
            chunk(t - 1)

        return carry

    lax.fori_loop(0, chunks + 1, step, 0)

    def columns(j):
        who = lax.rem(x + j, nx)
        return remote(
            w_out.at[:, pl.ds(pl.multiple_of(who * feats, feats), feats)],
            col_w.at[pl.ds(pl.multiple_of(x * width, width), width), :],
            w_send.at[j - 1],
            w_recv.at[j - 1],
            {"x": who},
        )

    def handed(j):
        rows = pl.ds(pl.multiple_of(lax.rem(x + nx - j, nx) * width, width), width)
        return remote(
            col_w.at[rows, :],
            col_w.at[rows, :],
            hand_send.at[j - 1],
            hand_recv.at[j - 1],
            {"c": 1 - c},
        )

    @pl.when(c == 0)
    def _():
        for j in range(1, nx):
            columns(j).start()


    def own_map(h):
        ext = state[h]
        keep = jnp.exp(logsum[h, 0:1, :])
        return (keep[:, :BLK] * eye - ext[:, :BLK], ext[:, BLK:], keep)

    swap = remote(sc_send, sc_recv, c_send.at[0], c_recv.at[0], {"c": 1 - c})
    give = remote(fin_send, sin, c_send.at[1], c_recv.at[1], {"c": 1 - c})

    @pl.when(c == 0)
    def _():
        for h in range(heads):
            l, b, keep = own_map(h)
            sc_send[h, 0:BLK, 0:BLK] = l
            sc_send[h, 0:BLK, BLK:] = b
            sc_send[h, BLK:, :] = jnp.broadcast_to(keep, (8, 2 * BLK))
        swap.start()
        reading(chunks - 2)
        reading(chunks - 1)
        swap.wait_send()
        for j in range(1, nx):
            columns(j).wait_recv()
            handed(j).start()
        for j in range(1, nx):
            columns(j).wait_send()
            handed(j).wait_send()
        give.wait_recv()

    zero = jnp.zeros((BLK, BLK), F32)
    one_row = jnp.ones((1, 2 * BLK), F32)
    identity = (zero, zero, one_row)
    each = range(heads)

    def put(buf, slot, m, h):
        l, b, keep = m
        buf[slot, h, 0:BLK, 0:BLK] = l.astype(BF16)
        buf[slot, h, 0:BLK, BLK:] = b.astype(BF16)
        hi, lo = halves(keep)
        tail = lax.broadcasted_iota(jnp.int32, (PRE, 2 * BLK), 0)
        buf[slot, h, BLK:, :] = jnp.where(
            tail == 0,
            jnp.broadcast_to(hi.astype(F32), (PRE, 2 * BLK)),
            jnp.broadcast_to(lo.astype(F32), (PRE, 2 * BLK)),
        ).astype(BF16)

    def get(buf, slot, h):
        tail = buf[slot, h, BLK:, :].astype(F32)
        return (
            buf[slot, h, 0:BLK, 0:BLK].astype(F32),
            buf[slot, h, 0:BLK, BLK:].astype(F32),
            tail[0:1] + tail[1:2],
        )

    def pieces(buf, slot, send, recv, j, who):
        made = []
        for h in each:
            for p, (at, rows) in enumerate(PIECES):
                made.append(
                    remote(
                        buf.at[slot, h, pl.ds(at, rows), :],
                        buf.at[slot, h, pl.ds(at, rows), :],
                        send.at[j, h, p],
                        recv.at[j, h, p],
                        who,
                    )
                )
        return made

    @pl.when(c == 1)
    def _():
        own = [own_map(h) for h in each]
        swap.wait_recv()
        map0 = [
            (sc_recv[h, 0:BLK, 0:BLK], sc_recv[h, 0:BLK, BLK:], sc_recv[h, BLK : BLK + 1, :])
            for h in each
        ]
        y1 = pieces(yb, y, y_send, y_recv, 0, {"y": up_y})
        y2 = pieces(yb, y, y_send, y_recv, 1, {"y": down_y})
        y3 = pieces(yb, down_y, y_send, y_recv, 2, {"y": up_y})
        many = len(PIECES)

        def of_head(copies, h):
            return copies[h * many : (h + 1) * many]

        for h in each:
            put(yb, y, compose(own[h], map0[h]), h)
            for a, b in zip(of_head(y1, h), of_head(y2, h)):
                a.start()
                b.start()
        reading(chunks - 2)
        for a, b in zip(y1, y3):
            a.wait_recv()
            b.start()

        ups, downs = nz // 2, nz - 1 - nz // 2
        up = [
            pieces(zb, lax.rem(z + nz - j, nz), z_send, z_recv, j, {"z": up_z})
            for j in range(ups)
        ]
        dn = [
            pieces(zb, lax.rem(z + j, nz), z_send, z_recv, ups + j, {"z": down_z})
            for j in range(downs)
        ]
        near = [identity] * heads
        low_state = [zero] * heads
        own_near = [identity] * heads
        def guarded(flag, copies, wait=False):
            @pl.when(flag)
            def _():
                for a in copies:
                    if wait:
                        a.wait_send()
                    else:
                        a.start()

        sends_up = [jnp.logical_and(z < last_z, z >= j) for j in range(ups)]
        sends_dn = [lax.rem(z + j, nz) < downs for j in range(downs)]

        @pl.when(z == 0)
        def _():
            pl.semaphore_wait(ready, 1)

        before_row = []
        for h in each:
            for b in of_head(y2, h) + of_head(y3, h):
                b.wait_recv()
            maps = [get(yb, j, h) for j in range(ny)]
            low_pair = compose(maps[1], maps[0], True, True)
            high_pair = compose(maps[3], maps[2], True, True)
            triple = compose(maps[2], low_pair, True)
            put(zb, z, compose(high_pair, low_pair), h)
            guarded(sends_up[0], of_head(up[0], h))
            guarded(sends_dn[0], of_head(dn[0], h))
            prefix = pick(y == 0, identity, maps[0])
            prefix = pick(y == 2, low_pair, prefix)
            prefix = pick(y == 3, triple, prefix)
            before_row.append(prefix)
        reading(chunks - 1)
        for j in range(ups):
            for p in range(len(up[0])):

                @pl.when(z > j)
                def _():
                    up[j][p].wait_recv()

                if j + 1 < ups:
                    guarded(sends_up[j + 1], [up[j + 1][p]])
                if j < downs:

                    @pl.when(lax.rem(z + 1 + j, nz) < downs)
                    def _():
                        dn[j][p].wait_recv()
                        if j + 1 < downs:
                            dn[j + 1][p].start()

            d = j + 1
            for h in each:
                got = pick(z - d >= 0, get(zb, lax.rem(z + nz - d, nz), h), identity)
                if d < ups:
                    near[h] = compose(near[h], got, False, True)
                    got = pick(z + d - nz >= 0, get(zb, lax.rem(z + d, nz), h), identity)
                    low_state[h] = apply_map(got, low_state[h], True)
                    if d == ups - 1:
                        near[h] = compose(before_row[h], near[h])
                        own_near[h] = compose(map0[h], near[h])
                else:
                    row_state = apply_map(got, low_state[h], True)
                    fin_send[h] = apply_map(near[h], row_state)
                    sin[h] = apply_map(own_near[h], row_state)
        give.start()
        give.wait_send()
        for group in [y1, y2, y3]:
            for a in group:
                a.wait_send()
        for j in range(ups):
            guarded(sends_up[j], up[j], True)
        for j in range(downs):
            guarded(sends_dn[j], dn[j], True)

    h_direct, h_relay = ring(hg, 0, hd_send, hd_recv, hf_send, hf_recv)
    starts = [right3(sin[h]) for h in range(heads)]
    for t in range(chunks):
        rows = slice(t * BLK, (t + 1) * BLK)
        for h in range(heads):
            part = prelim[h, rows, :]
            head_out = dot1(left3(part[:, :BLK]), starts[h]) + part[:, BLK:]
            scaled = head_out * lax.rsqrt(
                jnp.mean(head_out * head_out, axis=-1, keepdims=True) + NORM_FLOOR
            )
            cols = slice(h * BLK, (h + 1) * BLK)
            hg[x, rows, cols] = (scaled * gate[rows, cols]).astype(BF16)
        for way in range(2):
            h_direct(way, t).start()
    for t in range(chunks):
        for way in range(2):
            h_direct(way, t).wait_recv()
            h_relay(way, t).start()
    own_cols.wait()
    @pl.when(c == 1)
    def _():
        for j in range(1, nx):
            handed(j).wait_recv()

    for t in range(chunks):
        rows = slice(t * BLK, (t + 1) * BLK)
        for way in range(2):
            h_relay(way, t).wait_recv()
        rows_all = jnp.concatenate([hg[p, rows, :] for p in range(nx)], axis=1)
        out[rows, :] = dot1(rows_all, col_w[...]).astype(BF16)

    for way in range(2):
        for p in range(2):
            last(way, p).wait_send()
    @pl.when(has_after)
    def _():
        for i in range(nx):
            pre_copy(i).wait_send()

    for t in range(chunks):
        for way in range(2):
            if t < final:
                direct(way, t).wait_send()
            relay(way, t).wait_send()
            h_direct(way, t).wait_send()
            h_relay(way, t).wait_send()


def on_device(
    sizes,
    layer_in,
    query_weight,
    key_weight,
    value_weight,
    gate_weight,
    beta_weight,
    decay_weight,
    conv_weight,
    decay_log,
    beta_bias,
    decay_bias,
    norm_gain,
    out_weight,
):
    tokens, feats = layer_in.shape
    depth, width = query_weight.shape
    nz, ny, nx = sizes["z"], sizes["y"], sizes["x"]
    chunks = tokens // BLK
    heads = 2
    hbm = pl.BlockSpec(memory_space=pltpu.HBM)
    vmem = pl.BlockSpec(memory_space=pltpu.VMEM)
    dma = pltpu.SemaphoreType.DMA
    zc = nz - 1
    return pl.pallas_call(
        functools.partial(kernel, sizes),
        out_shape=pltpu.VMEM((tokens, feats), BF16),
        in_specs=[hbm] * 13,
        out_specs=vmem,
        scratch_shapes=[
            pltpu.VMEM((nx, tokens + PRE, feats), BF16),
            pltpu.VMEM((depth, 4 * width + BLK), BF16),
            pltpu.VMEM((nx * width, feats), BF16),
            pltpu.VMEM((heads, BLK, 2 * BLK), F32),
            pltpu.VMEM((heads, 8, 2 * BLK), F32),
            pltpu.VMEM((heads, tokens, 2 * BLK), F32),
            pltpu.VMEM((tokens, width), F32),
            pltpu.VMEM((nx, tokens, width), BF16),
            pltpu.VMEM((heads, BLK + 8, 2 * BLK), F32),
            pltpu.VMEM((heads, BLK + 8, 2 * BLK), F32),
            pltpu.VMEM((ny, heads, BLK + PRE, 2 * BLK), BF16),
            pltpu.VMEM((nz, heads, BLK + PRE, 2 * BLK), BF16),
            pltpu.VMEM((heads, BLK, BLK), F32),
            pltpu.VMEM((heads, BLK, BLK), F32),
            pltpu.VMEM((heads, depth), BF16),
            pltpu.VMEM((heads, depth), BF16),
            pltpu.VMEM((3, 4, width), F32),
            pltpu.VMEM((BLK,), F32),
            pltpu.SMEM((heads,), F32),
            pltpu.SMEM((heads,), F32),
            pltpu.SMEM((heads,), F32),
            pltpu.VMEM((chunks, BLK + PRE, width), F32),
            pltpu.VMEM((chunks, BLK, width), F32),
            pltpu.VMEM((chunks, 2, BLK, BLK), F32),
            pltpu.VMEM((chunks, heads, BLK, BLK), F32),
            pltpu.VMEM((chunks, heads, BLK, 2 * BLK), F32),
            pltpu.VMEM((chunks, heads, BLK, 2 * BLK), F32),
            dma((13,)),
            dma((nx,)),
            dma((nx,)),
            dma((2, chunks + 1)),
            dma((2, chunks + 1)),
            dma((2, chunks)),
            dma((2, chunks)),
            dma((nx - 1,)),
            dma((nx - 1,)),
            dma((nx - 1,)),
            dma((nx - 1,)),
            dma((2,)),
            dma((2,)),
            dma((3, heads, len(PIECES))),
            dma((3, heads, len(PIECES))),
            dma((zc, heads, len(PIECES))),
            dma((zc, heads, len(PIECES))),
            dma((2, chunks)),
            dma((2, chunks)),
            dma((2, chunks)),
            dma((2, chunks)),
            pltpu.SemaphoreType.REGULAR,
        ],
        compiler_params=pltpu.CompilerParams(
            collective_id=0, has_side_effects=True, vmem_limit_bytes=66519040
        ),
        name="layer",
    )(
        layer_in,
        query_weight,
        key_weight,
        value_weight,
        gate_weight,
        beta_weight.T,
        decay_weight.T,
        conv_weight.transpose(1, 0, 2),
        decay_log,
        beta_bias,
        decay_bias,
        norm_gain,
        out_weight,
    )


def solution(mesh):
    sizes = {"z": 8, "y": 4, "c": 2, "x": mesh.shape["head"]}
    finer = Mesh(
        mesh.devices.reshape(sizes["z"], sizes["y"], sizes["c"], sizes["x"]),
        ("z", "y", "c", "x"),
    )
    return jax.shard_map(
        functools.partial(on_device, sizes),
        mesh=finer,
        in_specs=(
            P(SEQ, "x"),
            P(None, "x"),
            P(None, "x"),
            P(None, "x"),
            P(None, "x"),
            P(None, "x"),
            P(None, "x"),
            P(None, None, "x"),
            P("x"),
            P("x"),
            P("x"),
            P(),
            P("x", None),
        ),
        out_specs=P(SEQ, "x"),
        check_vma=False,
    )
```

```python
import functools

import jax
import jax.numpy as jnp
from jax import lax
from jax.experimental import pallas as pl
from jax.experimental.pallas import tpu as pltpu
from jax.sharding import Mesh
from jax.sharding import PartitionSpec as P

F32 = jnp.float32
BF16 = jnp.bfloat16
MESH = pl.DeviceIdType.MESH
SEQ = ("z", "y", "c")
BLK = 128
HALF = BLK // 2
PRE = 16
SENT = 8
PIECES = ((0, 48), (48, 48), (96, 48))
NORM_FLOOR = 0.0001

NN = (((1,), (0,)), ((), ()))


def dot1(a, b):
    return lax.dot_general(a, b, NN, preferred_element_type=F32)


def halves(a):
    hi = a.astype(BF16)
    lo = (a - hi.astype(F32)).astype(BF16)
    return hi, lo


def left3(a):
    hi, lo = halves(a)
    return jnp.concatenate([hi, hi, lo], axis=1)


def right3(b):
    hi, lo = halves(b)
    return jnp.concatenate([hi, lo, hi], axis=0)


def dot3(a, b):
    return dot1(left3(a), right3(b))


def product(a, b, exact_a=False, exact_b=False):
    if exact_a and exact_b:
        return dot1(a.astype(BF16), b.astype(BF16))
    if exact_a:
        hi, lo = halves(b)
        a = a.astype(BF16)
        return dot1(jnp.concatenate([a, a], axis=1), jnp.concatenate([hi, lo], axis=0))
    if exact_b:
        hi, lo = halves(a)
        b = b.astype(BF16)
        return dot1(jnp.concatenate([hi, lo], axis=1), jnp.concatenate([b, b], axis=0))
    return dot3(a, b)


def sigmoid(v):
    return 1.0 / (1.0 + jnp.exp(-v))


def silu(v):
    return v / (1.0 + jnp.exp(-v))


def softplus(v):
    return jnp.maximum(v, 0.0) + jnp.log(1.0 + jnp.exp(-jnp.abs(v)))


def compose(later, earlier, *exact):
    l2, b2, c2 = later
    l1, b1, c1 = earlier
    moved = product(l2, jnp.concatenate([l1, b1], axis=1), *exact)
    width = l1.shape[1]
    return (
        c2[:, :width] * l1 + c1[:, :width] * l2 - moved[:, :width],
        c2[:, :width] * b1 + b2 - moved[:, width:],
        c1 * c2,
    )


def apply_map(m, state, *exact):
    l, b, c = m
    return c[:, : state.shape[1]] * state - product(l, state, *exact) + b


def pick(flag, m, other):
    return jax.tree.map(lambda a, b: jnp.where(flag, a, b), m, other)


def kernel(
    sizes,
    x_in,
    wq,
    wk,
    wv,
    wg,
    wb_in,
    wd_in,
    conv_in,
    decay_log_in,
    beta_bias_in,
    decay_bias_in,
    norm_gain_in,
    w_out,
    out,
    xg,
    w_all,
    col_w,
    state,
    logsum,
    prelim,
    gate,
    hg,
    sc_send,
    sc_recv,
    yb,
    zb,
    fin_send,
    sin,
    wb,
    wd,
    conv_w,
    norm_gain,
    decay_log,
    beta_bias,
    decay_bias,
    kept_total,
    kept_kt,
    kept_state,
    kept_u,
    load_sem,
    pre_send,
    pre_recv,
    d_send,
    d_recv,
    f_send,
    f_recv,
    w_send,
    w_recv,
    hand_send,
    hand_recv,
    c_send,
    c_recv,
    y_send,
    y_recv,
    z_send,
    z_recv,
    hd_send,
    hd_recv,
    hf_send,
    hf_recv,
    ready,
):
    nz, ny, nx = sizes["z"], sizes["y"], sizes["x"]
    z = lax.axis_index("z")
    y = lax.axis_index("y")
    c = lax.axis_index("c")
    x = lax.axis_index("x")
    tokens = x_in.shape[0]
    feats = x_in.shape[1]
    chunks = tokens // BLK
    heads = 2
    width = heads * BLK
    right, left = lax.rem(x + 1, nx), lax.rem(x + nx - 1, nx)
    far = lax.rem(x + 2, nx)
    count = nz * ny * 2
    here = (z * ny + y) * 2 + c
    after = lax.rem(here + 1, count)
    prior = lax.rem(here + count - 1, count)

    def place(s, xx):
        return {"z": s // (ny * 2), "y": lax.rem(s // 2, ny), "c": lax.rem(s, 2), "x": xx}

    xg[:, 0:PRE, :] = jnp.zeros((nx, PRE, feats), BF16)

    weights = (wq, wk, wv, wg)
    split = 2 * width + BLK
    places = (split, 0, width, split + width)
    loads = [pltpu.make_async_copy(x_in, xg.at[x, pl.ds(PRE, tokens), :], load_sem.at[0])]
    loads[0].start()
    for i, w in enumerate(weights):
        cp = pltpu.make_async_copy(
            w, w_all.at[:, pl.ds(places[i], width)], load_sem.at[1 + i]
        )
        cp.start()
        loads.append(cp)
    small_loads = (
        (wb_in, wb),
        (wd_in, wd),
        (conv_in, conv_w),
        (norm_gain_in, norm_gain),
        (decay_log_in, decay_log),
        (beta_bias_in, beta_bias),
        (decay_bias_in, decay_bias),
    )
    for i, (src, dst) in enumerate(small_loads):
        cp = pltpu.make_async_copy(src, dst, load_sem.at[6 + i])
        cp.start()
        loads.append(cp)
    own_cols = pltpu.make_async_copy(
        w_out.at[:, pl.ds(pl.multiple_of(x * feats, feats), feats)],
        col_w.at[pl.ds(pl.multiple_of(x * width, width), width), :],
        load_sem.at[5],
    )
    own_cols.start()

    barrier = pltpu.get_barrier_semaphore()
    up_y, down_y = lax.rem(y + 1, ny), lax.rem(y + ny - 1, ny)
    up_z, down_z = lax.rem(z + 1, nz), lax.rem(z + nz - 1, nz)
    last_z = nz - 1
    has_after = here < count - 1
    has_prior = here > 0

    def enter(who):
        pl.semaphore_signal(barrier, inc=1, device_id=who, device_id_type=MESH)

    always = [{"x": right}, {"x": left}, {"x": far}, {"c": 1 - c}, {"y": up_y}, {"y": down_y}]
    for who in always:
        enter(who)

    @pl.when(has_prior)
    def _():
        for i in range(nx):
            enter(place(prior, i))

    @pl.when(z > 0)
    def _():
        enter({"z": down_z})

    @pl.when(z < last_z)
    def _():
        enter({"z": up_z})

    @pl.when(z == 0)
    def _():
        enter({"z": down_z})

    expected = (
        len(always)
        + nx * has_after.astype(jnp.int32)
        + (z < last_z).astype(jnp.int32)
        + (z > 0).astype(jnp.int32)
        + (z == last_z).astype(jnp.int32)
    )

    state[...] = jnp.zeros_like(state)
    eye = (
        lax.broadcasted_iota(jnp.int32, (BLK, BLK), 0)
        == lax.broadcasted_iota(jnp.int32, (BLK, BLK), 1)
    ).astype(F32)
    for h in range(heads):
        state[h, :, 0:BLK] = eye
    logsum[...] = jnp.zeros_like(logsum)
    pl.semaphore_wait(barrier, expected)

    @pl.when(jnp.logical_and(z == last_z, c == 1))
    def _():
        pl.semaphore_signal(ready, inc=1, device_id={"z": up_z}, device_id_type=MESH)

    loads[0].wait()

    def remote(src, dst, send, recv, who):
        return pltpu.make_async_remote_copy(
            src_ref=src,
            dst_ref=dst,
            send_sem=send,
            recv_sem=recv,
            device_id=who,
            device_id_type=MESH,
        )


    def ring(buf, base, send, recv, relay_send, relay_recv):
        def direct(way, t):
            rows = pl.ds(pl.multiple_of(base + t * BLK, PRE), BLK)
            return remote(
                buf.at[x, rows, :],
                buf.at[x, rows, :],
                send.at[way, t],
                recv.at[way, t],
                {"x": (right, left)[way]},
            )

        def relay(way, t):
            rows = pl.ds(pl.multiple_of(base + t * BLK + way * HALF, PRE), HALF)
            source = (left, right)[way]
            return remote(
                buf.at[source, rows, :],
                buf.at[source, rows, :],
                relay_send.at[way, t],
                relay_recv.at[way, t],
                {"x": (right, left)[way]},
            )

        return direct, relay

    direct, relay = ring(xg, PRE, d_send, d_recv, f_send, f_recv)
    final = chunks - 1

    def last(way, p):
        half = way if p == 0 else 1 - way
        rows = pl.ds(PRE + final * BLK + half * HALF, HALF)
        return remote(
            xg.at[x, rows, :],
            xg.at[x, rows, :],
            d_send.at[way, final + p],
            d_recv.at[way, final + p],
            {"x": (right, left)[way]},
        )

    def pre_copy(i):
        return remote(
            xg.at[x, pl.ds(tokens + SENT, SENT), :],
            xg.at[x, pl.ds(SENT, SENT), :],
            pre_send.at[i],
            pre_recv.at[x],
            place(after, i),
        )

    @pl.when(has_after)
    def _():
        for i in range(nx):
            pre_copy(i).start()

    for t in range(2):
        for way in range(2):
            direct(way, t).start()
    for cp in loads[1:]:
        cp.wait()
    depth = wb.shape[1]
    wide_row = lax.broadcasted_iota(jnp.int32, (8, BLK), 0)
    for i in range(depth // BLK):
        cols = slice(i * BLK, (i + 1) * BLK)
        b_rows, d_rows = wb[:, cols].astype(F32), wd[:, cols].astype(F32)
        tile = jnp.where(wide_row == 0, b_rows[0:1], 0.0)
        tile = jnp.where(wide_row == 1, b_rows[1:2], tile)
        tile = jnp.where(wide_row == 2, d_rows[0:1], tile)
        tile = jnp.where(wide_row == 3, d_rows[1:2], tile)
        tile = jnp.concatenate([tile, jnp.zeros((BLK - 8, BLK), F32)], axis=0)
        w_all[cols, 2 * width : split] = jnp.transpose(tile).astype(BF16)

    row_i = lax.broadcasted_iota(jnp.int32, (BLK, BLK), 0)
    col_i = lax.broadcasted_iota(jnp.int32, (BLK, BLK), 1)
    differ = jnp.bitwise_xor(row_i, col_i)
    within = row_i >= col_i
    before = row_i > col_i

    lane = lax.broadcasted_iota(jnp.int32, (1, BLK), 1)
    bias_row = jnp.where(lane == 0, beta_bias[0], 0.0)
    bias_row = jnp.where(lane == 1, beta_bias[1], bias_row)
    bias_row = jnp.where(lane == 2, decay_bias[0], bias_row)
    bias_row = jnp.where(lane == 3, decay_bias[1], bias_row)
    rate_row = jnp.where(lane == 2, decay_log[0], -200.0)
    rate_row = jnp.exp(jnp.where(lane == 3, decay_log[1], rate_row))
    gain_row = norm_gain[...].reshape(1, BLK)

    def unit_rows(v):
        return v * lax.rsqrt(jnp.sum(v * v, axis=-1, keepdims=True) + 1.0)

    def mix_taps(which, values):
        taps = [
            jnp.concatenate([conv_w[i, s : s + 1, :] for i in which], axis=1)
            for s in range(4)
        ]
        mixed = taps[0] * values
        for s in range(1, 4):
            mixed = mixed + taps[s] * pltpu.roll(values, s, 0)
        return silu(mixed[PRE:])

    def projected(t, begin, end):
        start = t * BLK if isinstance(t, int) else pl.multiple_of(t * BLK, BLK)
        rows = pl.ds(start, BLK + PRE)
        xs = jnp.concatenate([xg[p, rows, :] for p in range(nx)], axis=1)
        raw = dot1(xs, w_all[:, begin:end])
        convolved = raw[:, : 2 * width] if begin == 0 else raw[:, :width]
        first = jnp.logical_and(here == 0, t == 0)
        ext_row = lax.broadcasted_iota(jnp.int32, convolved.shape, 0)
        return raw, jnp.where(jnp.logical_and(first, ext_row < PRE), 0.0, convolved)

    def chunk(t):
        raw, kv = projected(t, 0, split)
        mixed = mix_taps((1, 2), kv)
        small = raw[PRE:, 2 * width :] + bias_row
        betas = sigmoid(small)
        steps = -rate_row * softplus(small)
        s_hi = steps.astype(BF16)
        rest = steps - s_hi.astype(F32)
        s_mid = rest.astype(BF16)
        s_lo = (rest - s_mid.astype(F32)).astype(BF16)
        tri = within.astype(F32).astype(BF16)
        total = dot1(
            jnp.concatenate([tri, tri, tri], axis=1),
            jnp.concatenate([s_hi, s_mid, s_lo], axis=0),
        )
        total_t = jnp.transpose(total)
        kept_total[t, 0] = total
        kept_total[t, 1] = total_t
        both = []
        for h in range(heads):
            k = unit_rows(mixed[:, h * BLK : (h + 1) * BLK])
            v = mixed[:, width + h * BLK : width + (h + 1) * BLK]
            beta = betas[:, h : h + 1]
            run_c = total[:, 2 + h : 3 + h]
            run_r = total_t[2 + h : 3 + h, :]
            end = run_r[:, BLK - 1 : BLK]
            decay = jnp.where(within, jnp.exp(jnp.minimum(run_c - run_r, 0.0)), 0.0)
            kt = jnp.transpose(k)
            low = jnp.where(before, beta * decay * dot3(k, kt), 0.0)
            ext = state[h]
            read = dot3((beta * jnp.exp(run_c)) * k, ext)
            right_side = jnp.concatenate([jnp.zeros_like(v), beta * v], axis=1) - read
            kept_kt[t, h] = kt
            kept_state[t, h] = ext
            both.append((low, right_side, kt, run_r, end, ext))
        first_links = [jnp.where(differ == 1, b[0], 0.0) for b in both]
        inv = [jnp.where(row_i == col_i, 1.0, 0.0) - m for m in first_links]
        rest = []
        for b, m in zip(both, first_links):
            later = jnp.where(differ > 1, b[0], 0.0)
            rest.append(later - product(later, m, False, True))
        w = 2
        while w < BLK:
            linking = jnp.logical_and(differ >= w, differ < 2 * w)
            links = [jnp.where(linking, r, 0.0) for r in rest]
            if 2 * w < BLK:
                later = [jnp.where(differ >= 2 * w, r, 0.0) for r in rest]
                stacked = [
                    jnp.concatenate([r, a], axis=0) for r, a in zip(later, inv)
                ]
                moved = [
                    s - product(s, m, False, True) for s, m in zip(stacked, links)
                ]
                rest = [m[:BLK] for m in moved]
                inv = [m[BLK:] for m in moved]
            else:
                inv = [a - product(a, m, False, True) for a, m in zip(inv, links)]
            w *= 2
        for h in range(heads):
            low, right_side, kt, run_r, end, ext = both[h]
            solved = dot3(inv[h], right_side)
            kept_u[t, h] = solved
            weighted = kt * jnp.exp(end - run_r)
            state[h] = jnp.exp(end) * ext + dot3(weighted, solved)
            logsum[h] = logsum[h] + jnp.broadcast_to(end, logsum.shape[1:])

    def reading(t):
        start = t * BLK if isinstance(t, int) else pl.multiple_of(t * BLK, BLK)
        out_rows = pl.ds(start, BLK)
        raw, q_rows = projected(t, split, split + 2 * width)
        gates = silu(raw[PRE:, width:])
        mixed = mix_taps((0,), q_rows)
        total, total_t = kept_total[t, 0], kept_total[t, 1]
        for h in range(heads):
            cols = slice(h * BLK, (h + 1) * BLK)
            gate[out_rows, cols] = gates[:, cols] * gain_row
            q = unit_rows(mixed[:, cols])
            run_c = total[:, 2 + h : 3 + h]
            run_r = total_t[2 + h : 3 + h, :]
            decay = jnp.where(within, jnp.exp(jnp.minimum(run_c - run_r, 0.0)), 0.0)
            mix = decay * dot3(q, kept_kt[t, h])
            prelim[h, out_rows, :] = dot3(jnp.exp(run_c) * q, kept_state[t, h]) + dot3(
                mix, kept_u[t, h]
            )

    def step(t, carry):
        @pl.when(t < final)
        def _():
            direct(0, t).wait_recv()
            direct(1, t).wait_recv()

        @pl.when(t == final)
        def _():
            last(0, 0).wait_recv()
            last(1, 0).wait_recv()

        @pl.when(t < chunks)
        def _():
            relay(0, t).start()
            relay(1, t).start()

        @pl.when(t < final - 2)
        def _():
            direct(0, t + 2).start()
            direct(1, t + 2).start()

        @pl.when(t == final - 2)
        def _():
            last(0, 0).start()
            last(1, 0).start()

        @pl.when(t == final - 1)
        def _():
            last(0, 1).start()
            last(1, 1).start()

        @pl.when(t == chunks)
        def _():
            last(0, 1).wait_recv()
            last(1, 1).wait_recv()

        @pl.when(jnp.logical_and(t == 0, has_prior))
        def _():
            for i in range(nx):
                remote(
                    xg.at[i, pl.ds(tokens + SENT, SENT), :],
                    xg.at[i, pl.ds(SENT, SENT), :],
                    pre_send.at[i],
                    pre_recv.at[i],
                    place(after, i),
                ).wait_recv()

        @pl.when(jnp.logical_and(t > 1, t < chunks))
        def _():
            reading(t - 2)

        @pl.when(t > 0)
        def _():
            relay(0, t - 1).wait_recv()
            relay(1, t - 1).wait_recv()
            chunk(t - 1)

        return carry

    lax.fori_loop(0, chunks + 1, step, 0)

    def columns(j):
        who = lax.rem(x + j, nx)
        return remote(
            w_out.at[:, pl.ds(pl.multiple_of(who * feats, feats), feats)],
            col_w.at[pl.ds(pl.multiple_of(x * width, width), width), :],
            w_send.at[j - 1],
            w_recv.at[j - 1],
            {"x": who},
        )

    def handed(j):
        rows = pl.ds(pl.multiple_of(lax.rem(x + nx - j, nx) * width, width), width)
        return remote(
            col_w.at[rows, :],
            col_w.at[rows, :],
            hand_send.at[j - 1],
            hand_recv.at[j - 1],
            {"c": 1 - c},
        )

    @pl.when(c == 0)
    def _():
        for j in range(1, nx):
            columns(j).start()


    def own_map(h):
        ext = state[h]
        keep = jnp.exp(logsum[h, 0:1, :])
        return (keep[:, :BLK] * eye - ext[:, :BLK], ext[:, BLK:], keep)

    swap = remote(sc_send, sc_recv, c_send.at[0], c_recv.at[0], {"c": 1 - c})
    give = remote(fin_send, sin, c_send.at[1], c_recv.at[1], {"c": 1 - c})

    @pl.when(c == 0)
    def _():
        for h in range(heads):
            l, b, keep = own_map(h)
            sc_send[h, 0:BLK, 0:BLK] = l
            sc_send[h, 0:BLK, BLK:] = b
            sc_send[h, BLK:, :] = jnp.broadcast_to(keep, (8, 2 * BLK))
        swap.start()
        reading(chunks - 2)
        reading(chunks - 1)
        swap.wait_send()
        for j in range(1, nx):
            columns(j).wait_recv()
            handed(j).start()
        for j in range(1, nx):
            columns(j).wait_send()
            handed(j).wait_send()
        give.wait_recv()

    zero = jnp.zeros((BLK, BLK), F32)
    one_row = jnp.ones((1, 2 * BLK), F32)
    identity = (zero, zero, one_row)
    each = range(heads)

    def put(buf, slot, m, h):
        l, b, keep = m
        buf[slot, h, 0:BLK, 0:BLK] = l.astype(BF16)
        buf[slot, h, 0:BLK, BLK:] = b.astype(BF16)
        hi, lo = halves(keep)
        tail = lax.broadcasted_iota(jnp.int32, (PRE, 2 * BLK), 0)
        buf[slot, h, BLK:, :] = jnp.where(
            tail == 0,
            jnp.broadcast_to(hi.astype(F32), (PRE, 2 * BLK)),
            jnp.broadcast_to(lo.astype(F32), (PRE, 2 * BLK)),
        ).astype(BF16)

    def get(buf, slot, h):
        tail = buf[slot, h, BLK:, :].astype(F32)
        return (
            buf[slot, h, 0:BLK, 0:BLK].astype(F32),
            buf[slot, h, 0:BLK, BLK:].astype(F32),
            tail[0:1] + tail[1:2],
        )

    def pieces(buf, slot, send, recv, j, who):
        made = []
        for h in each:
            for p, (at, rows) in enumerate(PIECES):
                made.append(
                    remote(
                        buf.at[slot, h, pl.ds(at, rows), :],
                        buf.at[slot, h, pl.ds(at, rows), :],
                        send.at[j, h, p],
                        recv.at[j, h, p],
                        who,
                    )
                )
        return made

    @pl.when(c == 1)
    def _():
        own = [own_map(h) for h in each]
        swap.wait_recv()
        map0 = [
            (sc_recv[h, 0:BLK, 0:BLK], sc_recv[h, 0:BLK, BLK:], sc_recv[h, BLK : BLK + 1, :])
            for h in each
        ]
        y1 = pieces(yb, y, y_send, y_recv, 0, {"y": up_y})
        y2 = pieces(yb, y, y_send, y_recv, 1, {"y": down_y})
        y3 = pieces(yb, down_y, y_send, y_recv, 2, {"y": up_y})
        many = len(PIECES)

        def of_head(copies, h):
            return copies[h * many : (h + 1) * many]

        for h in each:
            put(yb, y, compose(own[h], map0[h]), h)
            for a, b in zip(of_head(y1, h), of_head(y2, h)):
                a.start()
                b.start()
        reading(chunks - 2)
        for a, b in zip(y1, y3):
            a.wait_recv()
            b.start()

        ups, downs = nz // 2, nz - 1 - nz // 2
        up = [
            pieces(zb, lax.rem(z + nz - j, nz), z_send, z_recv, j, {"z": up_z})
            for j in range(ups)
        ]
        dn = [
            pieces(zb, lax.rem(z + j, nz), z_send, z_recv, ups + j, {"z": down_z})
            for j in range(downs)
        ]
        near = [identity] * heads
        low_state = [zero] * heads
        own_near = [identity] * heads
        def guarded(flag, copies, wait=False):
            @pl.when(flag)
            def _():
                for a in copies:
                    if wait:
                        a.wait_send()
                    else:
                        a.start()

        sends_up = [jnp.logical_and(z < last_z, z >= j) for j in range(ups)]
        sends_dn = [lax.rem(z + j, nz) < downs for j in range(downs)]

        @pl.when(z == 0)
        def _():
            pl.semaphore_wait(ready, 1)

        before_row = []
        for h in each:
            for b in of_head(y2, h) + of_head(y3, h):
                b.wait_recv()
            maps = [get(yb, j, h) for j in range(ny)]
            low_pair = compose(maps[1], maps[0], True, True)
            high_pair = compose(maps[3], maps[2], True, True)
            triple = compose(maps[2], low_pair, True)
            put(zb, z, compose(high_pair, low_pair), h)
            guarded(sends_up[0], of_head(up[0], h))
            guarded(sends_dn[0], of_head(dn[0], h))
            prefix = pick(y == 0, identity, maps[0])
            prefix = pick(y == 2, low_pair, prefix)
            prefix = pick(y == 3, triple, prefix)
            before_row.append(prefix)
        reading(chunks - 1)
        for j in range(ups):
            for p in range(len(up[0])):

                @pl.when(z > j)
                def _():
                    up[j][p].wait_recv()

                if j + 1 < ups:
                    guarded(sends_up[j + 1], [up[j + 1][p]])
                if j < downs:

                    @pl.when(lax.rem(z + 1 + j, nz) < downs)
                    def _():
                        dn[j][p].wait_recv()
                        if j + 1 < downs:
                            dn[j + 1][p].start()

            d = j + 1
            for h in each:
                got = pick(z - d >= 0, get(zb, lax.rem(z + nz - d, nz), h), identity)
                if d < ups:
                    near[h] = compose(near[h], got, False, True)
                    got = pick(z + d - nz >= 0, get(zb, lax.rem(z + d, nz), h), identity)
                    low_state[h] = apply_map(got, low_state[h], True)
                    if d == ups - 1:
                        near[h] = compose(before_row[h], near[h])
                        own_near[h] = compose(map0[h], near[h])
                else:
                    row_state = apply_map(got, low_state[h], True)
                    fin_send[h] = apply_map(near[h], row_state)
                    sin[h] = apply_map(own_near[h], row_state)
        give.start()
        give.wait_send()
        for group in [y1, y2, y3]:
            for a in group:
                a.wait_send()
        for j in range(ups):
            guarded(sends_up[j], up[j], True)
        for j in range(downs):
            guarded(sends_dn[j], dn[j], True)

    h_direct, h_relay = ring(hg, 0, hd_send, hd_recv, hf_send, hf_recv)
    starts = [right3(sin[h]) for h in range(heads)]
    for t in range(chunks):
        rows = slice(t * BLK, (t + 1) * BLK)
        for h in range(heads):
            part = prelim[h, rows, :]
            head_out = dot1(left3(part[:, :BLK]), starts[h]) + part[:, BLK:]
            scaled = head_out * lax.rsqrt(
                jnp.mean(head_out * head_out, axis=-1, keepdims=True) + NORM_FLOOR
            )
            cols = slice(h * BLK, (h + 1) * BLK)
            hg[x, rows, cols] = (scaled * gate[rows, cols]).astype(BF16)
        for way in range(2):
            h_direct(way, t).start()
    for t in range(chunks):
        for way in range(2):
            h_direct(way, t).wait_recv()
            h_relay(way, t).start()
    own_cols.wait()
    @pl.when(c == 1)
    def _():
        for j in range(1, nx):
            handed(j).wait_recv()

    for t in range(chunks):
        rows = slice(t * BLK, (t + 1) * BLK)
        for way in range(2):
            h_relay(way, t).wait_recv()
        rows_all = jnp.concatenate([hg[p, rows, :] for p in range(nx)], axis=1)
        out[rows, :] = dot1(rows_all, col_w[...]).astype(BF16)

    for way in range(2):
        for p in range(2):
            last(way, p).wait_send()
    @pl.when(has_after)
    def _():
        for i in range(nx):
            pre_copy(i).wait_send()

    for t in range(chunks):
        for way in range(2):
            if t < final:
                direct(way, t).wait_send()
            relay(way, t).wait_send()
            h_direct(way, t).wait_send()
            h_relay(way, t).wait_send()


def on_device(
    sizes,
    layer_in,
    query_weight,
    key_weight,
    value_weight,
    gate_weight,
    beta_weight,
    decay_weight,
    conv_weight,
    decay_log,
    beta_bias,
    decay_bias,
    norm_gain,
    out_weight,
):
    tokens, feats = layer_in.shape
    depth, width = query_weight.shape
    nz, ny, nx = sizes["z"], sizes["y"], sizes["x"]
    chunks = tokens // BLK
    heads = 2
    hbm = pl.BlockSpec(memory_space=pltpu.HBM)
    vmem = pl.BlockSpec(memory_space=pltpu.VMEM)
    dma = pltpu.SemaphoreType.DMA
    zc = nz - 1
    return pl.pallas_call(
        functools.partial(kernel, sizes),
        out_shape=pltpu.VMEM((tokens, feats), BF16),
        in_specs=[hbm] * 13,
        out_specs=vmem,
        scratch_shapes=[
            pltpu.VMEM((nx, tokens + PRE, feats), BF16),
            pltpu.VMEM((depth, 4 * width + BLK), BF16),
            pltpu.VMEM((nx * width, feats), BF16),
            pltpu.VMEM((heads, BLK, 2 * BLK), F32),
            pltpu.VMEM((heads, 8, 2 * BLK), F32),
            pltpu.VMEM((heads, tokens, 2 * BLK), F32),
            pltpu.VMEM((tokens, width), F32),
            pltpu.VMEM((nx, tokens, width), BF16),
            pltpu.VMEM((heads, BLK + 8, 2 * BLK), F32),
            pltpu.VMEM((heads, BLK + 8, 2 * BLK), F32),
            pltpu.VMEM((ny, heads, BLK + PRE, 2 * BLK), BF16),
            pltpu.VMEM((nz, heads, BLK + PRE, 2 * BLK), BF16),
            pltpu.VMEM((heads, BLK, BLK), F32),
            pltpu.VMEM((heads, BLK, BLK), F32),
            pltpu.VMEM((heads, depth), BF16),
            pltpu.VMEM((heads, depth), BF16),
            pltpu.VMEM((3, 4, width), F32),
            pltpu.VMEM((BLK,), F32),
            pltpu.SMEM((heads,), F32),
            pltpu.SMEM((heads,), F32),
            pltpu.SMEM((heads,), F32),
            pltpu.VMEM((chunks, 2, BLK, BLK), F32),
            pltpu.VMEM((chunks, heads, BLK, BLK), F32),
            pltpu.VMEM((chunks, heads, BLK, 2 * BLK), F32),
            pltpu.VMEM((chunks, heads, BLK, 2 * BLK), F32),
            dma((13,)),
            dma((nx,)),
            dma((nx,)),
            dma((2, chunks + 1)),
            dma((2, chunks + 1)),
            dma((2, chunks)),
            dma((2, chunks)),
            dma((nx - 1,)),
            dma((nx - 1,)),
            dma((nx - 1,)),
            dma((nx - 1,)),
            dma((2,)),
            dma((2,)),
            dma((3, heads, len(PIECES))),
            dma((3, heads, len(PIECES))),
            dma((zc, heads, len(PIECES))),
            dma((zc, heads, len(PIECES))),
            dma((2, chunks)),
            dma((2, chunks)),
            dma((2, chunks)),
            dma((2, chunks)),
            pltpu.SemaphoreType.REGULAR,
        ],
        compiler_params=pltpu.CompilerParams(
            collective_id=0, has_side_effects=True, vmem_limit_bytes=66519040
        ),
        name="layer",
    )(
        layer_in,
        query_weight,
        key_weight,
        value_weight,
        gate_weight,
        beta_weight.T,
        decay_weight.T,
        conv_weight.transpose(1, 0, 2),
        decay_log,
        beta_bias,
        decay_bias,
        norm_gain,
        out_weight,
    )


def solution(mesh):
    sizes = {"z": 8, "y": 4, "c": 2, "x": mesh.shape["head"]}
    finer = Mesh(
        mesh.devices.reshape(sizes["z"], sizes["y"], sizes["c"], sizes["x"]),
        ("z", "y", "c", "x"),
    )
    return jax.shard_map(
        functools.partial(on_device, sizes),
        mesh=finer,
        in_specs=(
            P(SEQ, "x"),
            P(None, "x"),
            P(None, "x"),
            P(None, "x"),
            P(None, "x"),
            P(None, "x"),
            P(None, "x"),
            P(None, None, "x"),
            P("x"),
            P("x"),
            P("x"),
            P(),
            P("x", None),
        ),
        out_specs=P(SEQ, "x"),
        check_vma=False,
    )
```
